512 devices in a mesh: grp: 2 (over y), ka: 16 (over z), ga: 8 (over x), ba: 2 (over core).
Axes of the slice: x: 8, y: 2, z: 16, core: 2. Of those that a mesh axis runs over, the one named last changes fastest.
The devices are a block of a 8x16x16 slice.
Arguments:
- coefficients: bfloat16 [2, 2, 64, 512, 9216], P(None, None, ('grp', 'ka'), 'ba', 'ga'), parts along dimension 2, may hold values from -1 to 1
- occupied: int32 [2, 64], P(None, ('grp', 'ka')), parts along dimension 1, may hold values from 64 to 512
- kweights: float32 [64], P(('grp', 'ka')), parts along dimension 0, may hold values from 0.5 to 2
- owner_map: int32 [1024], P('grp'), parts along dimension 0, may hold values from 0 to 31, as said below
- species: int32 [1024], P('grp'), parts along dimension 0, may hold values from 0 to 1
- positions: float32 [3, 1024], P(None, 'grp'), parts along dimension 1, may hold values from 0 to 100
- multipole: float32 [2, 9, 324], replicated, may hold values from -0.3125 to 0.3125
- widths: float32 [2], replicated, may hold values from 0.05 to 0.3
- potential: float32 [2, 1769472], P(None, ('grp', 'ga')), parts along dimension 1, may hold values from -0.0068359375 to 0.0068359375
Outputs:
- density: float32 [2, 2, 1024, 324], P(None, None, ('grp', 'ka', 'ga', 'ba')), parts along dimension 2
- forces: float32 [3, 1024], P(None, ('grp', 'ka', 'ga', 'ba')), parts along dimension 1
The draws below stay inside these ranges and needn't reach their ends.
There are 2 independent parts, one for each index of `grp`. The reference program is written for one: setup_inputs(seed, part) draws one part's arguments, and reference() takes and returns one part's arrays. A program takes and returns all parts, laid end to end along the dimension named above; an argument that names none is the same for every part. Nothing has to cross between parts.
Inputs may be any that keep to these rules, and one draw needn't show every extreme that they name: `owner_map`: within each aligned block of 64 atoms every owner number is named by exactly 2 atoms.
All inputs are finite; a program needn't handle non-finite values.
Results may differ from the reference program's by a relative error of at most 0.0003.
Values sent between devices are 32-bit elements; how exact they have to be, the bound alone decides.
No kernel may reach another device: no remote copies, remote signals or barrier semaphores. Data moves between devices by JAX's collectives and lax.ppermute only.
A program may use at most 64 MiB of HBM per device.

```python
import math
import jax
import jax.numpy as jnp
from jax import lax

NSPIN = 2
NPROJ = 18
ATOMS = 512
SPECIES = 2
NL = 9
GRID = 96
G_DEV = 110592
KPTS = 32
BANDS = 512
GTOT = 884736
ATOMS_BLK = 64
PER_OWN = 2
N_GA = 8
N_BA = 2


def draw_coefficients(key, part):
    keys = jax.random.split(key, 4)
    dims_all = (NSPIN, KPTS, BANDS, ATOMS, NPROJ)
    spread = (KPTS * BANDS) ** (-0.5)
    real_noise = jax.random.normal(keys[0], dims_all, jnp.float32)
    imag_noise = jax.random.normal(keys[1], dims_all, jnp.float32)
    mix_real = jax.random.normal(keys[2], (ATOMS, NPROJ, NPROJ), jnp.float32) / 6.0
    mix_imag = jax.random.normal(keys[3], (ATOMS, NPROJ, NPROJ), jnp.float32) / 6.0
    real_part = spread * (jnp.einsum('skbai,aij->skbaj', real_noise, mix_real) - jnp.einsum('skbai,aij->skbaj', imag_noise, mix_imag))
    imag_part = spread * (jnp.einsum('skbai,aij->skbaj', real_noise, mix_imag) + jnp.einsum('skbai,aij->skbaj', imag_noise, mix_real))
    stacked = jnp.stack([real_part, imag_part], axis=1).reshape(NSPIN, 2, KPTS, BANDS, ATOMS * NPROJ)
    return jnp.clip(stacked, -1.0, 1.0).astype(jnp.bfloat16)


def draw_owner_map(key, part):
    blocks = ATOMS // ATOMS_BLK

    def one_block(number):
        return jax.random.permutation(jax.random.fold_in(key, number), ATOMS_BLK)
    shuffled = jax.vmap(one_block)(jnp.arange(blocks, dtype=jnp.int32))
    return (shuffled // PER_OWN).reshape(ATOMS).astype(jnp.int32)


def place_ends(values, key, least, high):
    shape = values.shape
    index_at = [jax.random.randint(jax.random.fold_in(key, axis), (), 0, shape[axis]) for axis in range(len(shape))]
    values = values.at[tuple(index_at)].set(least)
    longest = shape.index(max(shape))
    index_at[longest] = (index_at[longest] + 1) % shape[longest]
    return values.at[tuple(index_at)].set(high)


def block_scale(stream_key, extent, cuts, smallest, high):
    gain, own = 1.0, jax.random.fold_in(stream_key, 6)
    for axis_at, parts in cuts:
        steps = jnp.exp(jax.random.uniform(jax.random.fold_in(own, axis_at), (parts,), jnp.float32, smallest / len(cuts), high / len(cuts)))
        gain = gain * jnp.repeat(steps, extent[axis_at] // parts).reshape([-1 if axis == axis_at else 1 for axis in range(len(extent))])
    return gain


def centred(rng, shape, width, reach, shards=(), kind=jnp.bfloat16):
    factor_of = block_scale(rng, shape, shards, -0.22, 0.18) if shards else 1.0
    array = jax.random.normal(rng, shape, jnp.float32) * width * factor_of
    return jnp.minimum(jnp.maximum(array, -reach), reach).astype(kind)


def setup_inputs(seed: int = 0, part: int = 0) -> dict:
    streams_of = jax.random.split(jax.random.key(seed), 10)
    part_splits = jax.random.split(jax.random.fold_in(streams_of[9], part), 10)
    return {
        "coefficients": draw_coefficients(jax.random.fold_in(jax.random.fold_in(streams_of[9], part), 71), part),
        "occupied": place_ends(jax.random.randint(part_splits[1], (NSPIN, KPTS), BANDS // 8, BANDS + 1), jax.random.fold_in(part_splits[1], 1), BANDS // 8, BANDS).astype(jnp.int32),
        "kweights": jnp.clip(jnp.exp(math.log(2.0) - 1.3862944 * jax.random.uniform(part_splits[2], (KPTS,), jnp.float32) ** block_scale(part_splits[2], (KPTS,), ((0, 16),), -0.2, 0.2)), 0.5, 2.0),
        "owner_map": draw_owner_map(jax.random.fold_in(jax.random.fold_in(streams_of[9], part), 71), part),
        "species": place_ends(jax.random.randint(part_splits[4], (ATOMS,), 0, SPECIES), jax.random.fold_in(part_splits[4], 1), 0, SPECIES - 1).astype(jnp.int32),
        "positions": jnp.clip(jax.random.uniform(part_splits[5], (3, ATOMS), jnp.float32, 0.0, 100.0), 0.0, 100.0),
        "multipole": centred(streams_of[6], (SPECIES, NL, NPROJ * NPROJ), (NPROJ * NPROJ) ** -0.5, 0.3125, (), jnp.float32),
        "widths": jnp.clip(jnp.exp(jax.random.uniform(streams_of[7], (SPECIES,), jnp.float32, math.log(0.05), math.log(0.3))), 0.05, 0.3),
        "potential": centred(part_splits[8], (2, GTOT), GTOT ** -0.5, 0.0068359375, ((1, 8),), jnp.float32),
    }


grid_step = 0.0625
highest = lax.Precision.HIGHEST


def harmonics(start_index, length, widths):
    indices = start_index + jnp.arange(length, dtype=jnp.int32)
    planes = [indices % GRID, (indices // GRID) % GRID, indices // (GRID * GRID)]
    vectors = []
    for plane_index in planes:
        signed = jnp.where(plane_index >= GRID // 2, plane_index - GRID, plane_index)
        vectors.append(grid_step * signed.astype(jnp.float32))
    along_x, along_y, along_z = vectors
    square = along_x * along_x + along_y * along_y + along_z * along_z
    shapes = jnp.stack([jnp.ones_like(square), along_x, along_y, along_z, along_x * along_y, along_y * along_z, along_z * along_x, along_x * along_x - along_y * along_y, 3.0 * along_z * along_z - square])
    damping = jnp.exp(-widths[:, None] * square[None, :])
    form_table = (damping[:, None, :] * shapes[None, :, :]).reshape(SPECIES * NL, length)
    return form_table, jnp.stack(vectors, axis=1)


def force_block(moments, places, form_table, vectors, pot_piece):
    smooth = jnp.dot(moments, form_table, precision=highest)
    phases = jnp.dot(places, vectors.T, precision=highest)
    wave_term = pot_piece[0][None, :] * jnp.sin(phases) + pot_piece[1][None, :] * jnp.cos(phases)
    return jnp.dot(smooth * wave_term, vectors, precision=highest)


def reference(coefficients, occupied, kweights, owner_map, species, positions, multipole, widths, potential):
    band_index = jnp.arange(BANDS, dtype=jnp.int32)
    band_masks = (band_index[None, None, :] < occupied[:, :, None]).astype(jnp.float32)

    def kpoint(running, inputs):
        kpoint_slab, band_mask, weight = inputs
        values = kpoint_slab.astype(jnp.float32).reshape(NSPIN, 2, BANDS, ATOMS, NPROJ)
        masked = values * band_mask[:, None, :, None, None]
        real_part = jnp.einsum("scnai,scnaj->saij", values, masked)
        cross_term = jnp.einsum("snai,snaj->saij", values[:, 0], masked[:, 1])
        imag_part = cross_term - jnp.swapaxes(cross_term, 2, 3)
        return running + weight * jnp.stack([real_part, imag_part], axis=1), None

    initial = jnp.zeros((NSPIN, 2, ATOMS, NPROJ, NPROJ), jnp.float32)
    density_all, unused = lax.scan(kpoint, initial, (jnp.moveaxis(coefficients, 2, 0), jnp.moveaxis(band_masks, 1, 0), kweights))
    density_all = density_all.reshape(NSPIN, 2, ATOMS, NPROJ * NPROJ)
    atom_index = jnp.arange(ATOMS, dtype=jnp.int32)
    sort_key = ((owner_map // N_BA) * N_GA + atom_index // ATOMS_BLK) * N_BA + owner_map % N_BA
    ordering = jnp.argsort(sort_key, stable=True).astype(jnp.int32)
    density = jnp.take(density_all, ordering, axis=2)
    real_total = jnp.sum(density_all[:, 0], axis=0)
    selector = (species[:, None] == jnp.arange(SPECIES, dtype=jnp.int32)[None, :]).astype(jnp.float32)
    moments = jnp.dot(real_total, multipole.reshape(SPECIES * NL, NPROJ * NPROJ).T, precision=highest) * jnp.repeat(selector, NL, axis=1)
    block_size = G_DEV // 8
    places = positions.T

    def gblock(running, number):
        start_index = number * block_size
        form_table, vectors = harmonics(start_index, block_size, widths)
        pot_piece = lax.dynamic_slice_in_dim(potential, start_index, block_size, 1)
        return running + force_block(moments, places, form_table, vectors, pot_piece), None

    force_all, unused = lax.scan(gblock, jnp.zeros((ATOMS, 3), jnp.float32), jnp.arange(GTOT // block_size, dtype=jnp.int32))
    forces = jnp.take(force_all, ordering, axis=0).T
    return density, forces
```

```python
import functools

import jax
import jax.numpy as jnp
import numpy as np
from jax import lax
from jax.experimental import pallas as pl
from jax.experimental.pallas import tpu as pltpu
from jax.sharding import PartitionSpec as P


NPROJ = 18
NL = 9
GRID = 96
LANES = 128
EDGE = 32
FOLD = 72
PACKED = NPROJ * NPROJ
WIDE = 384

grid_step = 0.0625

MONOMIALS = [
    (a, b, c) for a in range(4) for b in range(4) for c in range(4) if a + b + c <= 3
]
MONO_PAD = 32


def force_coefficients():
    shapes = [
        {(0, 0, 0): 1},
        {(1, 0, 0): 1},
        {(0, 1, 0): 1},
        {(0, 0, 1): 1},
        {(1, 1, 0): 1},
        {(0, 1, 1): 1},
        {(1, 0, 1): 1},
        {(2, 0, 0): 1, (0, 2, 0): -1},
        {(0, 0, 2): 2, (2, 0, 0): -1, (0, 2, 0): -1},
    ]
    table = np.zeros((16, LANES), np.float32)
    for l, terms in enumerate(shapes):
        for c in range(3):
            for powers, factor in terms.items():
                power = list(powers)
                power[c] += 1
                table[l, c * MONO_PAD + MONOMIALS.index(tuple(power))] += factor
    return table


def iota(shape, dim):
    return lax.broadcasted_iota(jnp.int32, shape, dim)


def div18(x):
    return (x * 3641) >> 16


def split(x):
    high = x.astype(jnp.bfloat16)
    return high, (x - high.astype(jnp.float32)).astype(jnp.bfloat16)


def dot_f32(a, b):
    return lax.dot_general(a, b, (((1,), (0,)), ((), ())), preferred_element_type=jnp.float32)


def gram_kernel(index, occ_ref, kw_ref, own_ref, x_ref, out_ref, xt_ref, acc_ref, y_ref):
    step = pl.program_id(0)
    spin, kpt = step // 2, step % 2
    bands, columns = x_ref.shape[3], x_ref.shape[4]
    tiles = columns // LANES
    kdim = 2 * bands

    @pl.when(step == 0)
    def _():
        acc_ref[...] = jnp.zeros_like(acc_ref)
        xt_ref[0:EDGE, :] = jnp.zeros((EDGE, kdim), jnp.bfloat16)
        xt_ref[EDGE + columns :, :] = jnp.zeros((EDGE, kdim), jnp.bfloat16)

    block, half, _ = index()
    count = occ_ref[spin, kpt] - half * bands
    mask = jnp.where(iota((bands, LANES), 0) < count, 1.0, 0.0).astype(jnp.bfloat16)
    weight = kw_ref[kpt]

    def turned(t):
        for c in range(2):
            block = x_ref[0, c, 0, :, t * LANES : (t + 1) * LANES]
            xt_ref[EDGE + t * LANES : EDGE + (t + 1) * LANES, c * bands : (c + 1) * bands] = block.T

    turned(0)
    for t in range(tiles):
        if t + 1 < tiles:
            turned(t + 1)
        real = x_ref[0, 0, 0, :, t * LANES : (t + 1) * LANES] * mask
        imag = x_ref[0, 1, 0, :, t * LANES : (t + 1) * LANES] * mask
        right = jnp.concatenate(
            [jnp.concatenate([real, imag], axis=1), jnp.concatenate([imag, -real], axis=1)], axis=0
        )
        left = xt_ref[t * LANES : (t + 1) * LANES + 2 * EDGE, :]
        gram = dot_f32(left, right)
        first = t * LANES - EDGE
        lane = iota((8, LANES), 1) + t * LANES
        rows = iota((8, LANES), 0)
        from_atom = rows - NPROJ * div18(lane)
        from_diagonal = rows - lane
        sums = [None] * (FOLD // 8)
        for v in range((LANES + 2 * EDGE) // 8):
            row = first + 8 * v
            if row < 0 or row >= columns:
                continue
            if row < t * LANES:
                value = gram[8 * v : 8 * v + 8, :LANES]
            elif row >= (t + 1) * LANES:
                value = gram[8 * v : 8 * v + 8, LANES:]
            else:
                value = jnp.where(
                    from_diagonal <= -row,
                    gram[8 * v : 8 * v + 8, :LANES],
                    gram[8 * v : 8 * v + 8, LANES:],
                )
            inside = (from_atom >= -row) & (from_atom < NPROJ - row)
            value = jnp.where(inside, value, 0.0)
            slot = (row // 8) % (FOLD // 8)
            sums[slot] = value if sums[slot] is None else sums[slot] + value
        for slot, value in enumerate(sums):
            acc_ref[spin, t, 8 * slot : 8 * slot + 8, :] += weight * value

    @pl.when(step == pl.num_programs(0) - 1)
    def _():
        own = own_ref[...]
        row = jnp.sum(jnp.where(iota(own.shape, 0) == block // 2, own, 0), axis=0, keepdims=True)
        row = jnp.where(block % 2 == 1, pltpu.roll(row, LANES // 2, 1), row)
        atoms = LANES // 2
        eye = iota((atoms, LANES), 0) == iota((atoms, LANES), 1)
        rowf = row.astype(jnp.float32)
        col = jnp.sum(jnp.where(eye, rowf, 0.0), axis=1, keepdims=True)
        earlier = (col == rowf) & (iota((atoms, LANES), 0) < iota((atoms, LANES), 1))
        slot = jnp.sum(jnp.where(earlier, 1.0, 0.0), axis=0, keepdims=True)
        place = rowf * 4.0 + slot
        place = jnp.where(iota((1, LANES), 1) < atoms, place, pltpu.roll(place, atoms, 1))
        out_row = iota((LANES, LANES), 0).astype(jnp.float32)
        picks = [
            jnp.where(place + 2.0 * s == out_row, 1.0, 0.0).astype(jnp.bfloat16) for s in range(2)
        ]
        pick = jnp.concatenate(picks, axis=1)
        parts = []
        for s in range(2):
            for t in range(tiles):
                folded = acc_ref[s, t, 0:24, :]
                for q in range(1, FOLD // NPROJ):
                    folded = folded + acc_ref[s, t, NPROJ * q : NPROJ * q + 24, :]
                padded = jnp.concatenate(
                    [folded, jnp.zeros((LANES - 24, LANES), jnp.float32)], axis=0
                )
                y_ref[t * LANES : (t + 1) * LANES, :] = padded.T
            lane = iota((atoms, LANES), 1)
            packed = [jnp.zeros((atoms, LANES), jnp.float32) for _ in range(WIDE // LANES)]
            for j in range(NPROJ):
                piece = y_ref[pl.ds(j, atoms, stride=NPROJ), :]
                start = NPROJ * j
                shift = start % LANES
                if shift:
                    piece = pltpu.roll(piece, shift, 1)
                tile = start // LANES
                here = (lane >= shift) & (lane < shift + NPROJ)
                packed[tile] = jnp.where(here, piece, packed[tile])
                if shift + NPROJ > LANES:
                    packed[tile + 1] = jnp.where(
                        lane < shift + NPROJ - LANES, piece, packed[tile + 1]
                    )
            high, low = split(jnp.concatenate(packed, axis=1))
            parts += [high, low]
        result = dot_f32(pick, jnp.concatenate(parts, axis=0))
        for owner in range(out_ref.shape[0]):
            out_ref[owner] = result[4 * owner : 4 * owner + 4]


def gram(index, occupied, kweights, owners, coefficients, interpret=False):
    spins, comps, kpts, bands, columns = coefficients.shape
    tiles = columns // LANES
    smem = pl.BlockSpec(memory_space=pltpu.SMEM)
    return pl.pallas_call(
        functools.partial(gram_kernel, index),
        grid=(spins * kpts,),
        in_specs=[
            smem,
            smem,
            pl.BlockSpec((4, LANES), lambda g: (0, 0)),
            pl.BlockSpec((1, comps, 1, bands, columns), lambda g: (g // 2, 0, g % 2, 0, 0)),
        ],
        out_specs=pl.BlockSpec((LANES // 4, 4, WIDE), lambda g: (0, 0, 0)),
        out_shape=jax.ShapeDtypeStruct((LANES // 4, 4, WIDE), jnp.float32),
        scratch_shapes=[
            pltpu.VMEM((columns + 2 * EDGE, comps * bands), jnp.bfloat16),
            pltpu.VMEM((spins, tiles, 80, LANES), jnp.float32),
            pltpu.VMEM((columns, LANES), jnp.float32),
        ],
        cost_estimate=pl.CostEstimate(
            flops=2 * spins * kpts * columns * 192 * 2 * 2 * bands,
            bytes_accessed=spins * comps * kpts * bands * columns * 2,
            transcendentals=0,
        ),
        name="gram",
        interpret=interpret,
    )(occupied, kweights, owners, coefficients)


def sin_turns(t):
    t = t - jnp.floor(t + 0.5)
    t = jnp.where(t > 0.25, 0.5 - t, jnp.where(t < -0.25, -0.5 - t, t))
    x = t * np.float32(2.0 * np.pi)
    x2 = x * x
    p = np.float32(-1.0 / 39916800.0)
    for c in (1.0 / 362880.0, -1.0 / 5040.0, 1.0 / 120.0, -1.0 / 6.0):
        p = p * x2 + np.float32(c)
    return x + x * x2 * p


def signed(index):
    return jnp.where(index >= GRID // 2, index - GRID, index).astype(jnp.float32)


def wave_kernel(index, widths_ref, own_ref, species_ref, pos_ref, pot_ref, out_ref, kinds_ref, uh_ref, ul_ref):
    lines = 4
    rows = pot_ref.shape[0] // 6
    planes = rows * lines // GRID
    group = GRID // lines
    block, _, mine = index()
    own = own_ref[...]
    atoms = 16

    def spread(a):
        return jnp.concatenate([jnp.broadcast_to(a[r : r + 1], (4, LANES)) for r in range(4)], axis=0)

    at, lane16 = iota((atoms, LANES), 0), iota((atoms, LANES), 1)
    hit = (spread(own) == mine) & (lane16 // 64 == (at // 2) % 2)
    lanef = lane16.astype(jnp.float32)
    low = jnp.min(jnp.where(hit, lanef, 1e9), axis=1, keepdims=True)
    high = jnp.max(jnp.where(hit, lanef, -1.0), axis=1, keepdims=True)
    chosen = lanef == jnp.where(at % 2 == 1, high, low)

    lane = iota((1, LANES), 1)
    alpha, imag = (lane // atoms) % 4, lane // 64

    def on_lanes(a):
        column = jnp.sum(jnp.where(chosen, a, 0.0), axis=1, keepdims=True)
        return jnp.sum(jnp.where(at == lane16 % atoms, column, 0.0), axis=0, keepdims=True)

    place = [
        on_lanes(
            jnp.concatenate(
                [
                    jnp.broadcast_to(pos_ref[c : c + 1, r * LANES : (r + 1) * LANES], (4, LANES))
                    for r in range(4)
                ],
                axis=0,
            )
        )
        for c in range(3)
    ]
    kind = on_lanes(spread(species_ref[...]).astype(jnp.float32))
    width = jnp.where(kind > 0.5, widths_ref[1], widths_ref[0])
    turns = [p * np.float32(grid_step / (2.0 * np.pi)) for p in place]

    def power(g, exponent):
        g2 = g * g
        return jnp.where(
            exponent == 0, 1.0, jnp.where(exponent == 1, g, jnp.where(exponent == 2, g2, g2 * g))
        )

    mx = signed(iota((GRID, LANES), 0))
    gx = mx * grid_step
    phase = mx * turns[0]
    phase = phase - jnp.floor(phase + 0.5)
    factor = jnp.exp(-width * (gx * gx)) * power(gx, alpha)
    uh_ref[...] = jnp.zeros_like(uh_ref)
    ul_ref[...] = jnp.zeros_like(ul_ref)
    for c in range(2):
        shift = jnp.where(imag == 0, 0.25 + 0.25 * c, 0.25 * c)
        h, l = split(sin_turns(phase + shift) * factor)
        for line in range(lines):
            r = c * WIDE + line * GRID
            uh_ref[r : r + GRID, line * LANES : (line + 1) * LANES] = h
            ul_ref[r : r + GRID, line * LANES : (line + 1) * LANES] = l

    pieces = [
        split(pot_ref[pl.ds(2 * k + c, rows, stride=6), :]) for c in range(2) for k in range(3)
    ]
    vh = jnp.concatenate([p[0] for p in pieces], axis=1)
    vl = jnp.concatenate([p[1] for p in pieces], axis=1)
    first = dot_f32(vh, uh_ref[...]) + dot_f32(vl, uh_ref[...]) + dot_f32(vh, ul_ref[...])

    def tiled(a):
        return jnp.concatenate([a] * lines, axis=1)

    my = signed(lines * iota((group, lines * LANES), 0) + iota((group, lines * LANES), 1) // LANES)
    gy = my * grid_step
    phase = my * tiled(turns[1])
    phase = phase - jnp.floor(phase + 0.5)
    shift = tiled(jnp.where(imag == 0, 0.0, 0.25))
    damp = jnp.exp(-tiled(width) * (gy * gy))
    y1 = sin_turns(phase + shift) * damp
    y2 = sin_turns(phase + shift + 0.25) * damp

    zi = iota((16, LANES), 0) + block * planes
    mz = signed(jnp.where(zi >= GRID, zi - GRID, zi))
    gz = mz * grid_step
    phase = mz * turns[2]
    phase = phase - jnp.floor(phase + 0.5)
    damp = jnp.exp(-width * (gz * gz))
    zs = sin_turns(phase) * damp
    zc = sin_turns(phase + 0.25) * damp

    sums = {}
    for z in range(planes):
        wave = y1 * tiled(zc[z : z + 1]) + y2 * tiled(zs[z : z + 1])
        term = first[z * group : (z + 1) * group] * wave
        gz_row = gz[z : z + 1]
        for b in range(4):
            if b:
                term = term * gy
            total = None
            for r in range(0, group, 8):
                for line in range(lines):
                    piece = term[r : r + 8, line * LANES : (line + 1) * LANES]
                    total = piece if total is None else total + piece
            for c in range(4 - b):
                if c:
                    total = total * gz_row
                sums[b, c] = total if z == 0 else sums[b, c] + total
    reduced = {k: jnp.sum(v, axis=0, keepdims=True) for k, v in sums.items()}
    which = iota((MONO_PAD, LANES), 0)
    table = jnp.zeros((MONO_PAD, LANES), jnp.float32)
    for m, (a, b, c) in enumerate(MONOMIALS):
        table = jnp.where((which == m) & (alpha == a), reduced[b, c], table)
    aux = jnp.where(which == 0, kind, 0.0)
    turned = jnp.concatenate([table, aux, jnp.zeros((64, LANES), jnp.float32)], axis=0).T
    result = turned[0:atoms]
    for g in range(1, LANES // atoms):
        result = result + turned[g * atoms : (g + 1) * atoms]
    lane = iota((atoms, LANES), 1)
    sent = jnp.where(lane < MONO_PAD, result, 0.0)
    kinds_ref[...] = result
    for row in range(4):
        line = sent[4 * row : 4 * row + 1]
        for k in range(1, 4):
            line = line + pltpu.roll(sent[4 * row + k : 4 * row + k + 1], MONO_PAD * k, 1)
        out_ref[row : row + 1, :] = line


def waves(index, widths, owners, species, positions, potential, interpret=False):
    smem = pl.BlockSpec(memory_space=pltpu.SMEM)
    vmem = pl.BlockSpec(memory_space=pltpu.VMEM)
    return pl.pallas_call(
        functools.partial(wave_kernel, index),
        in_specs=[smem, vmem, vmem, vmem, vmem],
        out_specs=(vmem, vmem),
        out_shape=(
            jax.ShapeDtypeStruct((4, LANES), jnp.float32),
            jax.ShapeDtypeStruct((16, LANES), jnp.float32),
        ),
        scratch_shapes=[pltpu.VMEM((2 * WIDE, 4 * LANES), jnp.bfloat16)] * 2,
        cost_estimate=pl.CostEstimate(
            flops=2 * 288 * 768 * 512 * 3, bytes_accessed=potential.size * 4, transcendentals=0
        ),
        compiler_params=pltpu.CompilerParams(vmem_limit_bytes=16 << 20),
        name="waves",
        interpret=interpret,
    )(widths, owners, species, positions, potential)


def final_kernel(index, parts_ref, sums_ref, kinds_ref, mult_ref, coef_ref, density_ref, forces_ref):
    total = parts_ref[0]
    for r in range(1, parts_ref.shape[0]):
        total = total + parts_ref[r]
    z = jnp.concatenate([total, total], axis=0)
    r = iota((WIDE, WIDE), 0)
    u = div18(r)
    swap = (iota((WIDE, WIDE), 1) == (r - NPROJ * u) * NPROJ + u) & (r < PACKED)
    swap = jnp.where(swap, 1.0, 0.0).astype(jnp.bfloat16)
    high = z.astype(jnp.bfloat16)
    rest = z - high.astype(jnp.float32)
    middle = rest.astype(jnp.bfloat16)
    low = (rest - middle.astype(jnp.float32)).astype(jnp.bfloat16)
    turned = dot_f32(high, swap) + dot_f32(middle, swap) + dot_f32(low, swap)
    e = iota((8, WIDE), 1)
    u = div18(e)
    v = e - NPROJ * u
    real = jnp.where(v <= u, z, turned)
    imag = jnp.where(u > v, turned, jnp.where(u < v, -z, 0.0))
    for s in range(2):
        density_ref[s, 0] = real[2 * s : 2 * s + 2, :PACKED]
        density_ref[s, 1] = imag[2 * s : 2 * s + 2, :PACKED]

    both = real + pltpu.roll(real, 2, 0)
    block = index()[0]
    line = jnp.broadcast_to(sums_ref[pl.ds(block // 2, 1), :], (8, LANES))
    lane, row = iota((8, LANES), 1), iota((8, LANES), 0)
    line = jnp.where(block % 2 == 1, pltpu.roll(line, 2 * MONO_PAD, 1), line)
    line = jnp.where(row % 2 == 1, pltpu.roll(line, 3 * MONO_PAD, 1), line)
    line = jnp.where(lane < MONO_PAD, line, 0.0)
    sums = line + pltpu.roll(line, MONO_PAD, 1) + pltpu.roll(line, 2 * MONO_PAD, 1)
    kinds = jnp.concatenate([kinds_ref[pl.ds(2 * block, 2), :]] * 4, axis=0)
    kind = jnp.sum(jnp.where(lane == MONO_PAD, kinds, 0.0), axis=1, keepdims=True) > 4.0
    poly = jnp.zeros((8, LANES), jnp.float32)
    for l in range(NL):
        chosen = jnp.where(kind, mult_ref[l, 1:2, :], mult_ref[l, 0:1, :])
        moment = jnp.sum(both[:, :PACKED] * chosen, axis=1, keepdims=True)
        poly = poly + moment * coef_ref[l : l + 1, :]
    terms = poly * sums
    forces = jnp.concatenate(
        [
            jnp.sum(jnp.where(lane // MONO_PAD == c, terms, 0.0), axis=1, keepdims=True)
            for c in range(3)
        ],
        axis=1,
    )
    forces_ref[...] = forces[0:2, :]


def final(index, parts, sums, kinds, multipole, coefs, interpret=False):
    vmem = pl.BlockSpec(memory_space=pltpu.VMEM)
    return pl.pallas_call(
        functools.partial(final_kernel, index),
        in_specs=[vmem] * 5,
        out_specs=(vmem, vmem),
        out_shape=(
            jax.ShapeDtypeStruct((2, 2, 2, PACKED), jnp.float32),
            jax.ShapeDtypeStruct((2, 3), jnp.float32),
        ),
        cost_estimate=pl.CostEstimate(flops=10**7, bytes_accessed=10**5, transcendentals=0),
        compiler_params=pltpu.CompilerParams(vmem_limit_bytes=8 << 20),
        name="final",
        interpret=interpret,
    )(parts, sums, kinds, multipole, coefs)


def place():
    half = lax.axis_index("ba")
    return lax.axis_index("ga"), half, lax.axis_index("ka") * lax.axis_size("ba") + half


def step(
    coefficients, occupied, kweights, owner_map, species, positions, multipole, widths, potential
):
    owners = owner_map.reshape(4, LANES)
    packed = gram(place, occupied, kweights, owners, coefficients)
    packed, widths, positions, species, potential, multipole = lax.optimization_barrier(
        (packed, widths, positions, species, potential, multipole)
    )
    arrived = lax.all_to_all(packed, ("ka", "ba"), split_axis=0, concat_axis=0, tiled=True)
    values = potential.reshape(2, -1, LANES).transpose(1, 0, 2).reshape(-1, LANES)
    sums, kinds = waves(place, widths, owners, species.reshape(4, LANES), positions, values)
    sums = lax.psum(sums, "ga")
    density, forces = final(
        place, arrived, sums, kinds, multipole.transpose(1, 0, 2), jnp.asarray(force_coefficients())
    )
    return density, forces.T


def solution(mesh):
    placed = (
        P(None, None, ("grp", "ka"), "ba", "ga"),
        P(None, ("grp", "ka")),
        P(("grp", "ka")),
        P("grp"),
        P("grp"),
        P(None, "grp"),
        P(),
        P(),
        P(None, ("grp", "ga")),
    )
    return jax.shard_map(
        step,
        mesh=mesh,
        in_specs=placed,
        out_specs=(
            P(None, None, ("grp", "ka", "ga", "ba"), None),
            P(None, ("grp", "ka", "ga", "ba")),
        ),
        check_vma=False,
    )
```

```python
import functools

import jax
import jax.numpy as jnp
import numpy as np
from jax import lax
from jax.experimental import pallas as pl
from jax.experimental.pallas import tpu as pltpu
from jax.sharding import PartitionSpec as P


NPROJ = 18
NL = 9
GRID = 96
LANES = 128
EDGE = 16
FOLD = 72
PACKED = NPROJ * NPROJ
WIDE = 384

grid_step = 0.0625

MONOMIALS = [
    (a, b, c) for a in range(4) for b in range(4) for c in range(4) if a + b + c <= 3
]
MONO_PAD = 32
GRAM_VMEM = 60 << 20
FIRST = 4


def force_coefficients():
    shapes = [
        {(0, 0, 0): 1},
        {(1, 0, 0): 1},
        {(0, 1, 0): 1},
        {(0, 0, 1): 1},
        {(1, 1, 0): 1},
        {(0, 1, 1): 1},
        {(1, 0, 1): 1},
        {(2, 0, 0): 1, (0, 2, 0): -1},
        {(0, 0, 2): 2, (2, 0, 0): -1, (0, 2, 0): -1},
    ]
    table = np.zeros((16, LANES), np.float32)
    for l, terms in enumerate(shapes):
        for c in range(3):
            for powers, factor in terms.items():
                power = list(powers)
                power[c] += 1
                table[l, c * MONO_PAD + MONOMIALS.index(tuple(power))] += factor
    return table


def iota(shape, dim):
    return lax.broadcasted_iota(jnp.int32, shape, dim)


def div18(x):
    return (x * 3641) >> 16


def split(x):
    high = x.astype(jnp.bfloat16)
    return high, (x - high.astype(jnp.float32)).astype(jnp.bfloat16)


def dot_f32(a, b):
    return lax.dot_general(a, b, (((1,), (0,)), ((), ())), preferred_element_type=jnp.float32)


def gram_kernel(
    index, occ_hbm, kw_hbm, own_hbm, x_hbm, out_ref,
    occ_ref, kw_ref, own_ref, x_ref, xt_ref, acc_ref, y_ref, parts_ref, sems, small_sems,
):
    spins, comps, kpts, bands, columns = x_hbm.shape
    tiles = columns // LANES
    block, half, _ = index()

    cuts = [(0, 0, FIRST), (0, FIRST, tiles), (1, 0, tiles)]

    def arrivals(n):
        s, low, high = cuts[n]
        part = pl.ds(low * LANES, (high - low) * LANES)
        return [
            pltpu.make_async_copy(
                x_hbm.at[s, c, k, :, part], x_ref.at[s, c, k, :, part], sems.at[n, c, k]
            )
            for k in range(kpts)
            for c in range(comps)
        ]

    small = [
        pltpu.make_async_copy(src, dst, small_sems.at[n])
        for n, (src, dst) in enumerate(
            ((occ_hbm, occ_ref), (kw_hbm, kw_ref), (own_hbm, own_ref))
        )
    ]
    for copy in small:
        copy.start()
    for n in range(2):
        for copy in arrivals(n):
            copy.start()

    acc_ref[:, FOLD:, :] = jnp.zeros((tiles, 80 - FOLD, LANES), jnp.float32)
    edge = jnp.zeros((kpts, EDGE, comps * bands), jnp.bfloat16)
    xt_ref[:, 0:EDGE, :] = edge
    xt_ref[:, EDGE + columns :, :] = edge
    for copy in small:
        copy.wait()
    atoms = LANES // 2

    def spin_part(s):
        band = iota((1, comps * bands), 1) % bands
        masks = [
            jnp.where(band < occ_ref[s, k] - half * bands, 1.0, 0.0).astype(jnp.bfloat16)
            for k in range(kpts)
        ]

        def turned(t):
            for k in range(kpts):
                block_t = jnp.concatenate(
                    [x_ref[s, c, k, :, t * LANES : (t + 1) * LANES].T for c in range(comps)],
                    axis=1,
                )
                xt_ref[k, EDGE + t * LANES : EDGE + (t + 1) * LANES, :] = block_t * masks[k]

        def arrived(t):
            for n, cut in enumerate(cuts):
                if cut[:2] == (s, t):
                    for copy in arrivals(n):
                        copy.wait()
                    if n == 0:
                        for copy in arrivals(2):
                            copy.start()

        arrived(0)
        turned(0)
        for t in range(tiles):
            if t + 1 < tiles:
                arrived(t + 1)
                turned(t + 1)
            lane = iota((8, LANES), 1) + t * LANES
            rows = iota((8, LANES), 0)
            from_atom = rows - NPROJ * div18(lane)
            from_diagonal = rows - lane
            grams = []
            for k in range(kpts):
                real = x_ref[s, 0, k, :, t * LANES : (t + 1) * LANES]
                imag = x_ref[s, 1, k, :, t * LANES : (t + 1) * LANES]
                right = jnp.concatenate(
                    [
                        jnp.concatenate([real, imag], axis=1),
                        jnp.concatenate([imag, -real], axis=1),
                    ],
                    axis=0,
                )
                left = xt_ref[k, t * LANES : (t + 1) * LANES + 2 * EDGE, :]
                grams.append(dot_f32(left, right))
            first = t * LANES - EDGE
            sums = [None] * (FOLD // 8)
            for v in range((LANES + 2 * EDGE) // 8):
                row = first + 8 * v
                if row < 0 or row >= columns:
                    continue
                if row + 8 <= NPROJ * (t * LANES // NPROJ):
                    continue
                if row >= NPROJ * -(-(t + 1) * LANES // NPROJ):
                    continue
                if row < t * LANES:
                    parts = [g[8 * v : 8 * v + 8, :LANES] for g in grams]
                elif row >= (t + 1) * LANES:
                    parts = [g[8 * v : 8 * v + 8, LANES:] for g in grams]
                else:
                    upper = from_diagonal <= -row
                    parts = [
                        jnp.where(upper, g[8 * v : 8 * v + 8, :LANES], g[8 * v : 8 * v + 8, LANES:])
                        for g in grams
                    ]
                value = parts[0] * kw_ref[0]
                for k in range(1, kpts):
                    value = value + parts[k] * kw_ref[k]
                inside = (from_atom >= -row) & (from_atom < NPROJ - row)
                value = jnp.where(inside, value, 0.0)
                at = (row // 8) % (FOLD // 8)
                sums[at] = value if sums[at] is None else sums[at] + value
            for at, value in enumerate(sums):
                acc_ref[t, 8 * at : 8 * at + 8, :] = value
            folded = acc_ref[t, 0:24, :]
            for q in range(1, FOLD // NPROJ):
                folded = folded + acc_ref[t, NPROJ * q : NPROJ * q + 24, :]
            padded = jnp.concatenate([folded, jnp.zeros((LANES - 24, LANES), jnp.float32)], axis=0)
            y_ref[t * LANES : (t + 1) * LANES, :] = padded.T
        lane = iota((atoms, LANES), 1)
        packed = [jnp.zeros((atoms, LANES), jnp.float32) for _ in range(WIDE // LANES)]
        for j in range(NPROJ):
            piece = y_ref[pl.ds(j, atoms, stride=NPROJ), :]
            start = NPROJ * j
            shift = start % LANES
            if shift:
                piece = pltpu.roll(piece, shift, 1)
            tile = start // LANES
            here = (lane >= shift) & (lane < shift + NPROJ)
            packed[tile] = jnp.where(here, piece, packed[tile])
            if shift + NPROJ > LANES:
                packed[tile + 1] = jnp.where(lane < shift + NPROJ - LANES, piece, packed[tile + 1])
        high, low = split(jnp.concatenate(packed, axis=1))
        parts_ref[s] = jnp.concatenate([high, low], axis=0)

    for s in range(spins):
        spin_part(s)

    own = own_ref[...]
    row = jnp.sum(jnp.where(iota(own.shape, 0) == block // 2, own, 0), axis=0, keepdims=True)
    row = jnp.where(block % 2 == 1, pltpu.roll(row, LANES // 2, 1), row)
    eye = iota((atoms, LANES), 0) == iota((atoms, LANES), 1)
    rowf = row.astype(jnp.float32)
    col = jnp.sum(jnp.where(eye, rowf, 0.0), axis=1, keepdims=True)
    earlier = (col == rowf) & (iota((atoms, LANES), 0) < iota((atoms, LANES), 1))
    slot = jnp.sum(jnp.where(earlier, 1.0, 0.0), axis=0, keepdims=True)
    place = rowf * 4.0 + slot
    place = jnp.where(iota((1, LANES), 1) < atoms, place, pltpu.roll(place, atoms, 1))
    out_row = iota((LANES, LANES), 0).astype(jnp.float32)
    pick = jnp.concatenate(
        [
            jnp.where(place + 2.0 * s == out_row, 1.0, 0.0).astype(jnp.bfloat16)
            for s in range(spins)
        ],
        axis=1,
    )
    result = dot_f32(pick, parts_ref[...].reshape(spins * LANES, WIDE))
    for owner in range(out_ref.shape[0]):
        out_ref[owner] = result[4 * owner : 4 * owner + 4]


def gram(index, occupied, kweights, owners, coefficients, interpret=False):
    spins, comps, kpts, bands, columns = coefficients.shape
    tiles = columns // LANES
    hbm = pl.BlockSpec(memory_space=pltpu.HBM)
    return pl.pallas_call(
        functools.partial(gram_kernel, index),
        in_specs=[hbm] * 4,
        out_specs=pl.BlockSpec(memory_space=pltpu.VMEM),
        out_shape=jax.ShapeDtypeStruct((LANES // 4, 4, WIDE), jnp.float32),
        scratch_shapes=[
            pltpu.SMEM(occupied.shape, jnp.int32),
            pltpu.SMEM(kweights.shape, jnp.float32),
            pltpu.VMEM(owners.shape, jnp.int32),
            pltpu.VMEM(coefficients.shape, jnp.bfloat16),
            pltpu.VMEM((kpts, columns + 2 * EDGE, comps * bands), jnp.bfloat16),
            pltpu.VMEM((tiles, 80, LANES), jnp.float32),
            pltpu.VMEM((columns, LANES), jnp.float32),
            pltpu.VMEM((spins, LANES, WIDE), jnp.bfloat16),
            pltpu.SemaphoreType.DMA((3, comps, kpts)),
            pltpu.SemaphoreType.DMA((3,)),
        ],
        compiler_params=pltpu.CompilerParams(vmem_limit_bytes=GRAM_VMEM),
        cost_estimate=pl.CostEstimate(
            flops=2 * spins * kpts * columns * 160 * 2 * 2 * bands,
            bytes_accessed=spins * comps * kpts * bands * columns * 2,
            transcendentals=0,
        ),
        name="gram",
        interpret=interpret,
    )(occupied, kweights, owners, coefficients)


def sin_turns(t):
    t = t - jnp.floor(t + 0.5)
    t = jnp.where(t > 0.25, 0.5 - t, jnp.where(t < -0.25, -0.5 - t, t))
    x = t * np.float32(2.0 * np.pi)
    x2 = x * x
    p = np.float32(-1.0 / 39916800.0)
    for c in (1.0 / 362880.0, -1.0 / 5040.0, 1.0 / 120.0, -1.0 / 6.0):
        p = p * x2 + np.float32(c)
    return x + x * x2 * p


def signed(index):
    return jnp.where(index >= GRID // 2, index - GRID, index).astype(jnp.float32)


def wave_kernel(index, widths_ref, own_ref, species_ref, pos_ref, pot_ref, out_ref, kinds_ref, uh_ref, ul_ref):
    lines = 4
    rows = pot_ref.shape[0] // 6
    planes = rows * lines // GRID
    group = GRID // lines
    block, _, mine = index()
    own = own_ref[...]
    atoms = 16

    def spread(a):
        return jnp.concatenate([jnp.broadcast_to(a[r : r + 1], (4, LANES)) for r in range(4)], axis=0)

    at, lane16 = iota((atoms, LANES), 0), iota((atoms, LANES), 1)
    hit = (spread(own) == mine) & (lane16 // 64 == (at // 2) % 2)
    lanef = lane16.astype(jnp.float32)
    low = jnp.min(jnp.where(hit, lanef, 1e9), axis=1, keepdims=True)
    high = jnp.max(jnp.where(hit, lanef, -1.0), axis=1, keepdims=True)
    chosen = lanef == jnp.where(at % 2 == 1, high, low)

    lane = iota((1, LANES), 1)
    alpha, imag = (lane // atoms) % 4, lane // 64

    def on_lanes(a):
        column = jnp.sum(jnp.where(chosen, a, 0.0), axis=1, keepdims=True)
        return jnp.sum(jnp.where(at == lane16 % atoms, column, 0.0), axis=0, keepdims=True)

    place = [
        on_lanes(
            jnp.concatenate(
                [
                    jnp.broadcast_to(pos_ref[c : c + 1, r * LANES : (r + 1) * LANES], (4, LANES))
                    for r in range(4)
                ],
                axis=0,
            )
        )
        for c in range(3)
    ]
    kind = on_lanes(spread(species_ref[...]).astype(jnp.float32))
    width = jnp.where(kind > 0.5, widths_ref[1], widths_ref[0])
    turns = [p * np.float32(grid_step / (2.0 * np.pi)) for p in place]

    def power(g, exponent):
        g2 = g * g
        return jnp.where(
            exponent == 0, 1.0, jnp.where(exponent == 1, g, jnp.where(exponent == 2, g2, g2 * g))
        )

    mx = signed(iota((GRID, LANES), 0))
    gx = mx * grid_step
    phase = mx * turns[0]
    phase = phase - jnp.floor(phase + 0.5)
    factor = jnp.exp(-width * (gx * gx)) * power(gx, alpha)
    uh_ref[...] = jnp.zeros_like(uh_ref)
    ul_ref[...] = jnp.zeros_like(ul_ref)
    for c in range(2):
        shift = jnp.where(imag == 0, 0.25 + 0.25 * c, 0.25 * c)
        h, l = split(sin_turns(phase + shift) * factor)
        for line in range(lines):
            r = c * WIDE + line * GRID
            uh_ref[r : r + GRID, line * LANES : (line + 1) * LANES] = h
            ul_ref[r : r + GRID, line * LANES : (line + 1) * LANES] = l

    pieces = [
        split(pot_ref[pl.ds(2 * k + c, rows, stride=6), :]) for c in range(2) for k in range(3)
    ]
    vh = jnp.concatenate([p[0] for p in pieces], axis=1)
    vl = jnp.concatenate([p[1] for p in pieces], axis=1)
    first = dot_f32(vh, uh_ref[...]) + dot_f32(vl, uh_ref[...]) + dot_f32(vh, ul_ref[...])

    def tiled(a):
        return jnp.concatenate([a] * lines, axis=1)

    my = signed(lines * iota((group, lines * LANES), 0) + iota((group, lines * LANES), 1) // LANES)
    gy = my * grid_step
    phase = my * tiled(turns[1])
    phase = phase - jnp.floor(phase + 0.5)
    shift = tiled(jnp.where(imag == 0, 0.0, 0.25))
    damp = jnp.exp(-tiled(width) * (gy * gy))
    y1 = sin_turns(phase + shift) * damp
    y2 = sin_turns(phase + shift + 0.25) * damp

    zi = iota((16, LANES), 0) + block * planes
    mz = signed(jnp.where(zi >= GRID, zi - GRID, zi))
    gz = mz * grid_step
    phase = mz * turns[2]
    phase = phase - jnp.floor(phase + 0.5)
    damp = jnp.exp(-width * (gz * gz))
    zs = sin_turns(phase) * damp
    zc = sin_turns(phase + 0.25) * damp

    sums = {}
    for z in range(planes):
        wave = y1 * tiled(zc[z : z + 1]) + y2 * tiled(zs[z : z + 1])
        term = first[z * group : (z + 1) * group] * wave
        gz_row = gz[z : z + 1]
        for b in range(4):
            if b:
                term = term * gy
            total = None
            for r in range(0, group, 8):
                for line in range(lines):
                    piece = term[r : r + 8, line * LANES : (line + 1) * LANES]
                    total = piece if total is None else total + piece
            for c in range(4 - b):
                if c:
                    total = total * gz_row
                sums[b, c] = total if z == 0 else sums[b, c] + total
    reduced = {k: jnp.sum(v, axis=0, keepdims=True) for k, v in sums.items()}
    which = iota((MONO_PAD, LANES), 0)
    table = jnp.zeros((MONO_PAD, LANES), jnp.float32)
    for m, (a, b, c) in enumerate(MONOMIALS):
        table = jnp.where((which == m) & (alpha == a), reduced[b, c], table)
    aux = jnp.where(which == 0, kind, 0.0)
    turned = jnp.concatenate([table, aux, jnp.zeros((64, LANES), jnp.float32)], axis=0).T
    result = turned[0:atoms]
    for g in range(1, LANES // atoms):
        result = result + turned[g * atoms : (g + 1) * atoms]
    lane = iota((atoms, LANES), 1)
    sent = jnp.where(lane < MONO_PAD, result, 0.0)
    kinds_ref[...] = result
    for row in range(4):
        line = sent[4 * row : 4 * row + 1]
        for k in range(1, 4):
            line = line + pltpu.roll(sent[4 * row + k : 4 * row + k + 1], MONO_PAD * k, 1)
        out_ref[row : row + 1, :] = line


def waves(index, widths, owners, species, positions, potential, interpret=False):
    smem = pl.BlockSpec(memory_space=pltpu.SMEM)
    vmem = pl.BlockSpec(memory_space=pltpu.VMEM)
    return pl.pallas_call(
        functools.partial(wave_kernel, index),
        in_specs=[smem, vmem, vmem, vmem, vmem],
        out_specs=(vmem, vmem),
        out_shape=(
            jax.ShapeDtypeStruct((4, LANES), jnp.float32),
            jax.ShapeDtypeStruct((16, LANES), jnp.float32),
        ),
        scratch_shapes=[pltpu.VMEM((2 * WIDE, 4 * LANES), jnp.bfloat16)] * 2,
        cost_estimate=pl.CostEstimate(
            flops=2 * 288 * 768 * 512 * 3, bytes_accessed=potential.size * 4, transcendentals=0
        ),
        compiler_params=pltpu.CompilerParams(vmem_limit_bytes=16 << 20),
        name="waves",
        interpret=interpret,
    )(widths, owners, species, positions, potential)


def final_kernel(index, parts_ref, sums_ref, kinds_ref, mult_ref, coef_ref, density_ref, forces_ref):
    total = parts_ref[0]
    for r in range(1, parts_ref.shape[0]):
        total = total + parts_ref[r]
    z = jnp.concatenate([total, total], axis=0)
    r = iota((WIDE, WIDE), 0)
    u = div18(r)
    swap = (iota((WIDE, WIDE), 1) == (r - NPROJ * u) * NPROJ + u) & (r < PACKED)
    swap = jnp.where(swap, 1.0, 0.0).astype(jnp.bfloat16)
    high = z.astype(jnp.bfloat16)
    rest = z - high.astype(jnp.float32)
    middle = rest.astype(jnp.bfloat16)
    low = (rest - middle.astype(jnp.float32)).astype(jnp.bfloat16)
    turned = dot_f32(high, swap) + dot_f32(middle, swap) + dot_f32(low, swap)
    e = iota((8, WIDE), 1)
    u = div18(e)
    v = e - NPROJ * u
    real = jnp.where(v <= u, z, turned)
    imag = jnp.where(u > v, turned, jnp.where(u < v, -z, 0.0))
    for s in range(2):
        density_ref[s, 0] = real[2 * s : 2 * s + 2, :PACKED]
        density_ref[s, 1] = imag[2 * s : 2 * s + 2, :PACKED]

    both = real + pltpu.roll(real, 2, 0)
    block = index()[0]
    line = jnp.broadcast_to(sums_ref[pl.ds(block // 2, 1), :], (8, LANES))
    lane, row = iota((8, LANES), 1), iota((8, LANES), 0)
    line = jnp.where(block % 2 == 1, pltpu.roll(line, 2 * MONO_PAD, 1), line)
    line = jnp.where(row % 2 == 1, pltpu.roll(line, 3 * MONO_PAD, 1), line)
    line = jnp.where(lane < MONO_PAD, line, 0.0)
    sums = line + pltpu.roll(line, MONO_PAD, 1) + pltpu.roll(line, 2 * MONO_PAD, 1)
    kinds = jnp.concatenate([kinds_ref[pl.ds(2 * block, 2), :]] * 4, axis=0)
    kind = jnp.sum(jnp.where(lane == MONO_PAD, kinds, 0.0), axis=1, keepdims=True) > 4.0
    poly = jnp.zeros((8, LANES), jnp.float32)
    for l in range(NL):
        chosen = jnp.where(kind, mult_ref[l, 1:2, :], mult_ref[l, 0:1, :])
        moment = jnp.sum(both[:, :PACKED] * chosen, axis=1, keepdims=True)
        poly = poly + moment * coef_ref[l : l + 1, :]
    terms = poly * sums
    forces = jnp.concatenate(
        [
            jnp.sum(jnp.where(lane // MONO_PAD == c, terms, 0.0), axis=1, keepdims=True)
            for c in range(3)
        ],
        axis=1,
    )
    forces_ref[...] = forces[0:2, :]


def final(index, parts, sums, kinds, multipole, coefs, interpret=False):
    vmem = pl.BlockSpec(memory_space=pltpu.VMEM)
    return pl.pallas_call(
        functools.partial(final_kernel, index),
        in_specs=[vmem] * 5,
        out_specs=(vmem, vmem),
        out_shape=(
            jax.ShapeDtypeStruct((2, 2, 2, PACKED), jnp.float32),
            jax.ShapeDtypeStruct((2, 3), jnp.float32),
        ),
        cost_estimate=pl.CostEstimate(flops=10**7, bytes_accessed=10**5, transcendentals=0),
        compiler_params=pltpu.CompilerParams(vmem_limit_bytes=8 << 20),
        name="final",
        interpret=interpret,
    )(parts, sums, kinds, multipole, coefs)


def place():
    half = lax.axis_index("ba")
    return lax.axis_index("ga"), half, lax.axis_index("ka") * lax.axis_size("ba") + half


def step(
    coefficients, occupied, kweights, owner_map, species, positions, multipole, widths, potential
):
    owners = owner_map.reshape(4, LANES)
    packed = gram(place, occupied, kweights, owners, coefficients)
    packed, widths, positions, species, potential, multipole = lax.optimization_barrier(
        (packed, widths, positions, species, potential, multipole)
    )
    arrived = lax.all_to_all(packed, ("ka", "ba"), split_axis=0, concat_axis=0, tiled=True)
    values = potential.reshape(2, -1, LANES).transpose(1, 0, 2).reshape(-1, LANES)
    sums, kinds = waves(place, widths, owners, species.reshape(4, LANES), positions, values)
    sums = lax.psum(sums, "ga")
    density, forces = final(
        place, arrived, sums, kinds, multipole.transpose(1, 0, 2), jnp.asarray(force_coefficients())
    )
    return density, forces.T


def solution(mesh):
    placed = (
        P(None, None, ("grp", "ka"), "ba", "ga"),
        P(None, ("grp", "ka")),
        P(("grp", "ka")),
        P("grp"),
        P("grp"),
        P(None, "grp"),
        P(),
        P(),
        P(None, ("grp", "ga")),
    )
    return jax.shard_map(
        step,
        mesh=mesh,
        in_specs=placed,
        out_specs=(
            P(None, None, ("grp", "ka", "ga", "ba"), None),
            P(None, ("grp", "ka", "ga", "ba")),
        ),
        check_vma=False,
    )
```

```python
import functools

import jax
import jax.numpy as jnp
import numpy as np
from jax import lax
from jax.experimental import pallas as pl
from jax.experimental.pallas import tpu as pltpu
from jax.sharding import PartitionSpec as P


NPROJ = 18
NL = 9
GRID = 96
LANES = 128
EDGE = 16
FOLD = 72
PACKED = NPROJ * NPROJ
WIDE = 384

grid_step = 0.0625

MONOMIALS = [
    (a, b, c) for a in range(4) for b in range(4) for c in range(4) if a + b + c <= 3
]
MONO_PAD = 32
GRAM_VMEM = 60 << 20
CHUNKS = 2
FIRST = 4


def force_coefficients():
    shapes = [
        {(0, 0, 0): 1},
        {(1, 0, 0): 1},
        {(0, 1, 0): 1},
        {(0, 0, 1): 1},
        {(1, 1, 0): 1},
        {(0, 1, 1): 1},
        {(1, 0, 1): 1},
        {(2, 0, 0): 1, (0, 2, 0): -1},
        {(0, 0, 2): 2, (2, 0, 0): -1, (0, 2, 0): -1},
    ]
    table = np.zeros((16, LANES), np.float32)
    for l, terms in enumerate(shapes):
        for c in range(3):
            for powers, factor in terms.items():
                power = list(powers)
                power[c] += 1
                table[l, c * MONO_PAD + MONOMIALS.index(tuple(power))] += factor
    return table


def swap_table():
    table = np.zeros((WIDE, WIDE), np.float32)
    e = np.arange(PACKED)
    table[e, e % NPROJ * NPROJ + e // NPROJ] = 1.0
    return table


def iota(shape, dim):
    return lax.broadcasted_iota(jnp.int32, shape, dim)


def div18(x):
    return (x * 3641) >> 16


def split(x):
    high = x.astype(jnp.bfloat16)
    return high, (x - high.astype(jnp.float32)).astype(jnp.bfloat16)


def dot_f32(a, b):
    return lax.dot_general(a, b, (((1,), (0,)), ((), ())), preferred_element_type=jnp.float32)


def gram_kernel(
    index, occ_hbm, kw_hbm, own_hbm, x_hbm, out_ref,
    occ_ref, kw_ref, own_ref, x_ref, xt_ref, acc_ref, y_ref, parts_ref, sems, small_sems,
):
    spins, comps, kpts, bands, columns = x_hbm.shape
    tiles = columns // LANES
    block, half, _ = index()

    cuts = [(0, 0, FIRST), (0, FIRST, tiles), (1, 0, tiles)]

    def arrivals(n):
        s, low, high = cuts[n]
        part = pl.ds(low * LANES, (high - low) * LANES)
        return [
            pltpu.make_async_copy(
                x_hbm.at[s, c, k, :, part], x_ref.at[s, c, k, :, part], sems.at[n, c, k]
            )
            for k in range(kpts)
            for c in range(comps)
        ]

    small = [
        pltpu.make_async_copy(src, dst, small_sems.at[n])
        for n, (src, dst) in enumerate(
            ((occ_hbm, occ_ref), (kw_hbm, kw_ref), (own_hbm, own_ref))
        )
    ]
    for copy in small:
        copy.start()
    for n in range(2):
        for copy in arrivals(n):
            copy.start()

    acc_ref[:, FOLD:, :] = jnp.zeros((tiles, 80 - FOLD, LANES), jnp.float32)
    edge = jnp.zeros((kpts, EDGE, comps * bands), jnp.bfloat16)
    xt_ref[:, 0:EDGE, :] = edge
    xt_ref[:, EDGE + columns :, :] = edge
    for copy in small:
        copy.wait()
    atoms = LANES // 2

    waited = set()

    def arrived(s, t):
        for n, cut in enumerate(cuts):
            if cut[:2] == (s, t) and n not in waited:
                waited.add(n)
                for copy in arrivals(n):
                    copy.wait()
                if n == 0:
                    for copy in arrivals(2):
                        copy.start()

    def spin_part(s):
        band = iota((1, comps * bands), 1) % bands
        masks = [
            jnp.where(band < occ_ref[s, k] - half * bands, 1.0, 0.0).astype(jnp.bfloat16)
            for k in range(kpts)
        ]

        def turned(t):
            for k in range(kpts):
                block_t = jnp.concatenate(
                    [x_ref[s, c, k, :, t * LANES : (t + 1) * LANES].T for c in range(comps)],
                    axis=1,
                )
                xt_ref[k, EDGE + t * LANES : EDGE + (t + 1) * LANES, :] = block_t * masks[k]

        arrived(s, 0)
        turned(0)
        for t in range(tiles):
            if t + 1 < tiles:
                arrived(s, t + 1)
                turned(t + 1)
            lane = iota((8, LANES), 1) + t * LANES
            rows = iota((8, LANES), 0)
            from_atom = rows - NPROJ * div18(lane)
            from_diagonal = rows - lane
            grams = []
            for k in range(kpts):
                real = x_ref[s, 0, k, :, t * LANES : (t + 1) * LANES]
                imag = x_ref[s, 1, k, :, t * LANES : (t + 1) * LANES]
                right = jnp.concatenate(
                    [
                        jnp.concatenate([real, imag], axis=1),
                        jnp.concatenate([imag, -real], axis=1),
                    ],
                    axis=0,
                )
                left = xt_ref[k, t * LANES : (t + 1) * LANES + 2 * EDGE, :]
                grams.append(dot_f32(left, right))
            first = t * LANES - EDGE
            sums = [None] * (FOLD // 8)
            for v in range((LANES + 2 * EDGE) // 8):
                row = first + 8 * v
                if row < 0 or row >= columns:
                    continue
                if row + 8 <= NPROJ * (t * LANES // NPROJ):
                    continue
                if row >= NPROJ * -(-(t + 1) * LANES // NPROJ):
                    continue
                if row < t * LANES:
                    parts = [g[8 * v : 8 * v + 8, :LANES] for g in grams]
                elif row >= (t + 1) * LANES:
                    parts = [g[8 * v : 8 * v + 8, LANES:] for g in grams]
                else:
                    upper = from_diagonal <= -row
                    parts = [
                        jnp.where(upper, g[8 * v : 8 * v + 8, :LANES], g[8 * v : 8 * v + 8, LANES:])
                        for g in grams
                    ]
                value = parts[0] * kw_ref[0]
                for k in range(1, kpts):
                    value = value + parts[k] * kw_ref[k]
                inside = (from_atom >= -row) & (from_atom < NPROJ - row)
                value = jnp.where(inside, value, 0.0)
                at = (row // 8) % (FOLD // 8)
                sums[at] = value if sums[at] is None else sums[at] + value
            for at, value in enumerate(sums):
                acc_ref[t, 8 * at : 8 * at + 8, :] = value
            folded = acc_ref[t, 0:24, :]
            for q in range(1, FOLD // NPROJ):
                folded = folded + acc_ref[t, NPROJ * q : NPROJ * q + 24, :]
            padded = jnp.concatenate([folded, jnp.zeros((LANES - 24, LANES), jnp.float32)], axis=0)
            y_ref[t * LANES : (t + 1) * LANES, :] = padded.T
        lane = iota((atoms, LANES), 1)
        packed = [jnp.zeros((atoms, LANES), jnp.float32) for _ in range(WIDE // LANES)]
        for j in range(NPROJ):
            piece = y_ref[pl.ds(j, atoms, stride=NPROJ), :]
            start = NPROJ * j
            shift = start % LANES
            if shift:
                piece = pltpu.roll(piece, shift, 1)
            tile = start // LANES
            here = (lane >= shift) & (lane < shift + NPROJ)
            packed[tile] = jnp.where(here, piece, packed[tile])
            if shift + NPROJ > LANES:
                packed[tile + 1] = jnp.where(lane < shift + NPROJ - LANES, piece, packed[tile + 1])
        high, low = split(jnp.concatenate(packed, axis=1))
        parts_ref[s] = jnp.concatenate([high, low], axis=0)

    for s in range(spins):
        spin_part(s)

    own = own_ref[...]
    row = jnp.sum(jnp.where(iota(own.shape, 0) == block // 2, own, 0), axis=0, keepdims=True)
    row = jnp.where(block % 2 == 1, pltpu.roll(row, LANES // 2, 1), row)
    eye = iota((atoms, LANES), 0) == iota((atoms, LANES), 1)
    rowf = row.astype(jnp.float32)
    col = jnp.sum(jnp.where(eye, rowf, 0.0), axis=1, keepdims=True)
    earlier = (col == rowf) & (iota((atoms, LANES), 0) < iota((atoms, LANES), 1))
    slot = jnp.sum(jnp.where(earlier, 1.0, 0.0), axis=0, keepdims=True)
    place = rowf * 4.0 + slot
    place = jnp.where(iota((1, LANES), 1) < atoms, place, pltpu.roll(place, atoms, 1))
    out_row = iota((LANES, LANES), 0).astype(jnp.float32)
    pick = jnp.concatenate(
        [
            jnp.where(place + 2.0 * s == out_row, 1.0, 0.0).astype(jnp.bfloat16)
            for s in range(spins)
        ],
        axis=1,
    )
    result = dot_f32(pick, parts_ref[...].reshape(spins * LANES, WIDE))
    for owner in range(out_ref.shape[0]):
        out_ref[owner] = result[4 * owner : 4 * owner + 4]


def gram(index, occupied, kweights, owners, coefficients, interpret=False):
    spins, comps, kpts, bands, columns = coefficients.shape
    tiles = columns // LANES
    hbm = pl.BlockSpec(memory_space=pltpu.HBM)
    return pl.pallas_call(
        functools.partial(gram_kernel, index),
        in_specs=[hbm] * 4,
        out_specs=pl.BlockSpec(memory_space=pltpu.VMEM),
        out_shape=jax.ShapeDtypeStruct((LANES // 4, 4, WIDE), jnp.float32),
        scratch_shapes=[
            pltpu.SMEM(occupied.shape, jnp.int32),
            pltpu.SMEM(kweights.shape, jnp.float32),
            pltpu.VMEM(owners.shape, jnp.int32),
            pltpu.VMEM(coefficients.shape, jnp.bfloat16),
            pltpu.VMEM((kpts, columns + 2 * EDGE, comps * bands), jnp.bfloat16),
            pltpu.VMEM((tiles, 80, LANES), jnp.float32),
            pltpu.VMEM((columns, LANES), jnp.float32),
            pltpu.VMEM((spins, LANES, WIDE), jnp.bfloat16),
            pltpu.SemaphoreType.DMA((3, comps, kpts)),
            pltpu.SemaphoreType.DMA((3,)),
        ],
        compiler_params=pltpu.CompilerParams(vmem_limit_bytes=GRAM_VMEM),
        cost_estimate=pl.CostEstimate(
            flops=2 * spins * kpts * columns * 160 * 2 * 2 * bands,
            bytes_accessed=spins * comps * kpts * bands * columns * 2,
            transcendentals=0,
        ),
        name="gram",
        interpret=interpret,
    )(occupied, kweights, owners, coefficients)


def sin_turns(t):
    t = t - jnp.floor(t + 0.5)
    t = jnp.where(t > 0.25, 0.5 - t, jnp.where(t < -0.25, -0.5 - t, t))
    x = t * np.float32(2.0 * np.pi)
    x2 = x * x
    p = np.float32(-1.0 / 39916800.0)
    for c in (1.0 / 362880.0, -1.0 / 5040.0, 1.0 / 120.0, -1.0 / 6.0):
        p = p * x2 + np.float32(c)
    return x + x * x2 * p


def signed(index):
    return jnp.where(index >= GRID // 2, index - GRID, index).astype(jnp.float32)


def wave_kernel(index, widths_ref, own_ref, species_ref, pos_ref, pot_ref, out_ref, kinds_ref, uh_ref, ul_ref):
    lines = 4
    rows = pot_ref.shape[0] // 6
    planes = rows * lines // GRID
    group = GRID // lines
    block, _, mine = index()
    own = own_ref[...]
    atoms = 16

    def spread(a):
        return jnp.concatenate([jnp.broadcast_to(a[r : r + 1], (4, LANES)) for r in range(4)], axis=0)

    at, lane16 = iota((atoms, LANES), 0), iota((atoms, LANES), 1)
    hit = (spread(own) == mine) & (lane16 // 64 == (at // 2) % 2)
    lanef = lane16.astype(jnp.float32)
    low = jnp.min(jnp.where(hit, lanef, 1e9), axis=1, keepdims=True)
    high = jnp.max(jnp.where(hit, lanef, -1.0), axis=1, keepdims=True)
    chosen = lanef == jnp.where(at % 2 == 1, high, low)

    lane = iota((1, LANES), 1)
    alpha, imag = (lane // atoms) % 4, lane // 64

    def on_lanes(a):
        column = jnp.sum(jnp.where(chosen, a, 0.0), axis=1, keepdims=True)
        return jnp.sum(jnp.where(at == lane16 % atoms, column, 0.0), axis=0, keepdims=True)

    place = [
        on_lanes(
            jnp.concatenate(
                [
                    jnp.broadcast_to(pos_ref[c : c + 1, r * LANES : (r + 1) * LANES], (4, LANES))
                    for r in range(4)
                ],
                axis=0,
            )
        )
        for c in range(3)
    ]
    kind = on_lanes(spread(species_ref[...]).astype(jnp.float32))
    width = jnp.where(kind > 0.5, widths_ref[0:1, 1:2], widths_ref[0:1, 0:1])
    turns = [p * np.float32(grid_step / (2.0 * np.pi)) for p in place]

    def power(g, exponent):
        g2 = g * g
        return jnp.where(
            exponent == 0, 1.0, jnp.where(exponent == 1, g, jnp.where(exponent == 2, g2, g2 * g))
        )

    mx = signed(iota((GRID, LANES), 0))
    gx = mx * grid_step
    phase = mx * turns[0]
    phase = phase - jnp.floor(phase + 0.5)
    factor = jnp.exp(-width * (gx * gx)) * power(gx, alpha)
    uh_ref[...] = jnp.zeros_like(uh_ref)
    ul_ref[...] = jnp.zeros_like(ul_ref)
    for c in range(2):
        shift = jnp.where(imag == 0, 0.25 + 0.25 * c, 0.25 * c)
        h, l = split(sin_turns(phase + shift) * factor)
        for line in range(lines):
            side, place_in = line // 2, line % 2
            r = c * 2 * LANES + line * GRID - side * LANES
            n = place_in * LANES
            uh_ref[side, r : r + GRID, n : n + LANES] = h
            ul_ref[side, r : r + GRID, n : n + LANES] = l

    def lines_of(low, high):
        pieces = [
            [
                split(pot_ref[pl.ds(2 * k + c + 6 * low, high - low, stride=6), :])
                for k in range(3)
            ]
            for c in range(2)
        ]
        sides = []
        for side in range(2):
            vh = jnp.concatenate([pieces[c][side + k][0] for c in range(2) for k in range(2)], axis=1)
            vl = jnp.concatenate([pieces[c][side + k][1] for c in range(2) for k in range(2)], axis=1)
            uh, ul = uh_ref[side], ul_ref[side]
            sides.append(dot_f32(vh, uh) + dot_f32(vl, uh) + dot_f32(vh, ul))
        return jnp.concatenate(sides, axis=1)

    def tiled(a):
        return jnp.concatenate([a] * lines, axis=1)

    my = signed(lines * iota((group, lines * LANES), 0) + iota((group, lines * LANES), 1) // LANES)
    gy = my * grid_step
    phase = my * tiled(turns[1])
    phase = phase - jnp.floor(phase + 0.5)
    shift = tiled(jnp.where(imag == 0, 0.0, 0.25))
    damp = jnp.exp(-tiled(width) * (gy * gy))
    y1 = sin_turns(phase + shift) * damp
    y2 = sin_turns(phase + shift + 0.25) * damp

    zi = iota((16, LANES), 0) + block * planes
    mz = signed(jnp.where(zi >= GRID, zi - GRID, zi))
    gz = mz * grid_step
    phase = mz * turns[2]
    phase = phase - jnp.floor(phase + 0.5)
    damp = jnp.exp(-width * (gz * gz))
    zs = sin_turns(phase) * damp
    zc = sin_turns(phase + 0.25) * damp

    sums = {}
    chunk = planes // CHUNKS
    for z in range(planes):
        if z % chunk == 0:
            first = lines_of(z * group, (z + chunk) * group)
        wave = y1 * tiled(zc[z : z + 1]) + y2 * tiled(zs[z : z + 1])
        row = z % chunk * group
        term = first[row : row + group] * wave
        gz_row = gz[z : z + 1]
        for b in range(4):
            if b:
                term = term * gy
            total = None
            for r in range(0, group, 8):
                for line in range(lines):
                    piece = term[r : r + 8, line * LANES : (line + 1) * LANES]
                    total = piece if total is None else total + piece
            for c in range(4 - b):
                if c:
                    total = total * gz_row
                sums[b, c] = total if z == 0 else sums[b, c] + total
    reduced = {k: jnp.sum(v, axis=0, keepdims=True) for k, v in sums.items()}
    which = iota((MONO_PAD, LANES), 0)
    table = jnp.zeros((MONO_PAD, LANES), jnp.float32)
    for m, (a, b, c) in enumerate(MONOMIALS):
        table = jnp.where((which == m) & (alpha == a), reduced[b, c], table)
    aux = jnp.where(which == 0, kind, 0.0)
    turned = jnp.concatenate([table, aux, jnp.zeros((64, LANES), jnp.float32)], axis=0).T
    result = turned[0:atoms]
    for g in range(1, LANES // atoms):
        result = result + turned[g * atoms : (g + 1) * atoms]
    lane = iota((atoms, LANES), 1)
    sent = jnp.where(lane < MONO_PAD, result, 0.0)
    kinds_ref[...] = result
    for row in range(4):
        line = sent[4 * row : 4 * row + 1]
        for k in range(1, 4):
            line = line + pltpu.roll(sent[4 * row + k : 4 * row + k + 1], MONO_PAD * k, 1)
        out_ref[row : row + 1, :] = line


def waves(index, widths, owners, species, positions, potential, interpret=False):
    vmem = pl.BlockSpec(memory_space=pltpu.VMEM)
    return pl.pallas_call(
        functools.partial(wave_kernel, index),
        in_specs=[vmem] * 5,
        out_specs=(vmem, vmem),
        out_shape=(
            jax.ShapeDtypeStruct((4, LANES), jnp.float32),
            jax.ShapeDtypeStruct((16, LANES), jnp.float32),
        ),
        scratch_shapes=[pltpu.VMEM((2, 4 * LANES, 2 * LANES), jnp.bfloat16)] * 2,
        cost_estimate=pl.CostEstimate(
            flops=2 * 288 * 768 * 512 * 3, bytes_accessed=potential.size * 4, transcendentals=0
        ),
        compiler_params=pltpu.CompilerParams(vmem_limit_bytes=16 << 20),
        name="waves",
        interpret=interpret,
    )(widths.reshape(1, -1), owners, species, positions, potential)


def final_kernel(index, parts_ref, sums_ref, kinds_ref, swap_ref, mult_ref, coef_ref, density_ref, forces_ref):
    total = parts_ref[0]
    for r in range(1, parts_ref.shape[0]):
        total = total + parts_ref[r]
    z = jnp.concatenate([total, total], axis=0)
    swap = swap_ref[...]
    high = z.astype(jnp.bfloat16)
    rest = z - high.astype(jnp.float32)
    middle = rest.astype(jnp.bfloat16)
    low = (rest - middle.astype(jnp.float32)).astype(jnp.bfloat16)
    turned = dot_f32(high, swap) + dot_f32(middle, swap) + dot_f32(low, swap)
    e = iota((8, WIDE), 1)
    u = div18(e)
    v = e - NPROJ * u
    real = jnp.where(v <= u, z, turned)
    imag = jnp.where(u > v, turned, jnp.where(u < v, -z, 0.0))
    for s in range(2):
        density_ref[s, 0] = real[2 * s : 2 * s + 2, :PACKED]
        density_ref[s, 1] = imag[2 * s : 2 * s + 2, :PACKED]

    both = real + pltpu.roll(real, 2, 0)
    block = index()[0]
    line = jnp.broadcast_to(sums_ref[pl.ds(block // 2, 1), :], (8, LANES))
    lane, row = iota((8, LANES), 1), iota((8, LANES), 0)
    line = jnp.where(block % 2 == 1, pltpu.roll(line, 2 * MONO_PAD, 1), line)
    line = jnp.where(row % 2 == 1, pltpu.roll(line, 3 * MONO_PAD, 1), line)
    line = jnp.where(lane < MONO_PAD, line, 0.0)
    sums = line + pltpu.roll(line, MONO_PAD, 1) + pltpu.roll(line, 2 * MONO_PAD, 1)
    kinds = jnp.concatenate([kinds_ref[pl.ds(2 * block, 2), :]] * 4, axis=0)
    kind = jnp.sum(jnp.where(lane == MONO_PAD, kinds, 0.0), axis=1, keepdims=True) > 4.0
    poly = jnp.zeros((8, LANES), jnp.float32)
    for l in range(NL):
        chosen = jnp.where(kind, mult_ref[l, 1:2, :], mult_ref[l, 0:1, :])
        moment = jnp.sum(both[:, :PACKED] * chosen, axis=1, keepdims=True)
        poly = poly + moment * coef_ref[l : l + 1, :]
    terms = poly * sums
    forces = jnp.concatenate(
        [
            jnp.sum(jnp.where(lane // MONO_PAD == c, terms, 0.0), axis=1, keepdims=True)
            for c in range(3)
        ],
        axis=1,
    )
    forces_ref[...] = forces[0:2, :]


def final(index, parts, sums, kinds, swap, multipole, coefs, interpret=False):
    vmem = pl.BlockSpec(memory_space=pltpu.VMEM)
    return pl.pallas_call(
        functools.partial(final_kernel, index),
        in_specs=[vmem] * 6,
        out_specs=(vmem, vmem),
        out_shape=(
            jax.ShapeDtypeStruct((2, 2, 2, PACKED), jnp.float32),
            jax.ShapeDtypeStruct((2, 3), jnp.float32),
        ),
        cost_estimate=pl.CostEstimate(flops=10**7, bytes_accessed=10**5, transcendentals=0),
        compiler_params=pltpu.CompilerParams(vmem_limit_bytes=8 << 20),
        name="final",
        interpret=interpret,
    )(parts, sums, kinds, swap, multipole, coefs)


def place():
    half = lax.axis_index("ba")
    return lax.axis_index("ga"), half, lax.axis_index("ka") * lax.axis_size("ba") + half


def step(
    coefficients, occupied, kweights, owner_map, species, positions, multipole, widths, potential
):
    owners = owner_map.reshape(4, LANES)
    packed = gram(place, occupied, kweights, owners, coefficients)
    packed, widths, positions, species, potential, multipole = lax.optimization_barrier(
        (packed, widths, positions, species, potential, multipole)
    )
    arrived = lax.all_to_all(packed, ("ka", "ba"), split_axis=0, concat_axis=0, tiled=True)
    values = potential.reshape(2, -1, LANES).transpose(1, 0, 2).reshape(-1, LANES)
    sums, kinds = waves(place, widths, owners, species.reshape(4, LANES), positions, values)
    sums = lax.psum(sums, "ga")
    density, forces = final(
        place,
        arrived,
        sums,
        kinds,
        jnp.asarray(swap_table(), jnp.bfloat16),
        multipole.transpose(1, 0, 2),
        jnp.asarray(force_coefficients()),
    )
    return density, forces.T


def solution(mesh):
    placed = (
        P(None, None, ("grp", "ka"), "ba", "ga"),
        P(None, ("grp", "ka")),
        P(("grp", "ka")),
        P("grp"),
        P("grp"),
        P(None, "grp"),
        P(),
        P(),
        P(None, ("grp", "ga")),
    )
    return jax.shard_map(
        step,
        mesh=mesh,
        in_specs=placed,
        out_specs=(
            P(None, None, ("grp", "ka", "ga", "ba"), None),
            P(None, ("grp", "ka", "ga", "ba")),
        ),
        check_vma=False,
    )
```

```python
import functools

import jax
import jax.numpy as jnp
import numpy as np
from jax import lax
from jax.experimental import pallas as pl
from jax.experimental.pallas import tpu as pltpu
from jax.sharding import PartitionSpec as P


NPROJ = 18
NL = 9
GRID = 96
LANES = 128
EDGE = 16
FOLD = 72
PACKED = NPROJ * NPROJ
WIDE = 384

grid_step = 0.0625

MONOMIALS = [
    (a, b, c) for a in range(4) for b in range(4) for c in range(4) if a + b + c <= 3
]
MONO_PAD = 32
REST = PACKED - 2 * LANES
LINES = 11
GRAM_VMEM = 60 << 20
CHUNKS = 2
FIRST = 4


def force_coefficients():
    shapes = [
        {(0, 0, 0): 1},
        {(1, 0, 0): 1},
        {(0, 1, 0): 1},
        {(0, 0, 1): 1},
        {(1, 1, 0): 1},
        {(0, 1, 1): 1},
        {(1, 0, 1): 1},
        {(2, 0, 0): 1, (0, 2, 0): -1},
        {(0, 0, 2): 2, (2, 0, 0): -1, (0, 2, 0): -1},
    ]
    table = np.zeros((16, LANES), np.float32)
    for l, terms in enumerate(shapes):
        for c in range(3):
            for powers, factor in terms.items():
                power = list(powers)
                power[c] += 1
                table[l, c * MONO_PAD + MONOMIALS.index(tuple(power))] += factor
    return table


def swap_table():
    table = np.zeros((WIDE, WIDE), np.float32)
    e = np.arange(PACKED)
    table[e, e % NPROJ * NPROJ + e // NPROJ] = 1.0
    return table


def iota(shape, dim):
    return lax.broadcasted_iota(jnp.int32, shape, dim)


def div18(x):
    return (x * 3641) >> 16


def split(x):
    high = x.astype(jnp.bfloat16)
    return high, (x - high.astype(jnp.float32)).astype(jnp.bfloat16)


def dot_f32(a, b):
    return lax.dot_general(a, b, (((1,), (0,)), ((), ())), preferred_element_type=jnp.float32)


def gram_kernel(
    index, occ_hbm, kw_hbm, own_hbm, x_hbm, out_ref,
    occ_ref, kw_ref, own_ref, x_ref, xt_ref, acc_ref, y_ref, parts_ref, sems, small_sems,
):
    spins, comps, kpts, bands, columns = x_hbm.shape
    tiles = columns // LANES
    block, half, _ = index()

    cuts = [(0, 0, FIRST), (0, FIRST, tiles), (1, 0, tiles)]

    def arrivals(n):
        s, low, high = cuts[n]
        part = pl.ds(low * LANES, (high - low) * LANES)
        return [
            pltpu.make_async_copy(
                x_hbm.at[s, c, k, :, part], x_ref.at[s, c, k, :, part], sems.at[n, c, k]
            )
            for k in range(kpts)
            for c in range(comps)
        ]

    small = [
        pltpu.make_async_copy(src, dst, small_sems.at[n])
        for n, (src, dst) in enumerate(
            ((occ_hbm, occ_ref), (kw_hbm, kw_ref), (own_hbm, own_ref))
        )
    ]
    for copy in small:
        copy.start()
    for n in range(2):
        for copy in arrivals(n):
            copy.start()

    acc_ref[:, FOLD:, :] = jnp.zeros((tiles, 80 - FOLD, LANES), jnp.float32)
    edge = jnp.zeros((kpts, EDGE, comps * bands), jnp.bfloat16)
    xt_ref[:, 0:EDGE, :] = edge
    xt_ref[:, EDGE + columns :, :] = edge
    for copy in small:
        copy.wait()
    atoms = LANES // 2

    waited = set()

    def arrived(s, t):
        for n, cut in enumerate(cuts):
            if cut[:2] == (s, t) and n not in waited:
                waited.add(n)
                for copy in arrivals(n):
                    copy.wait()
                if n == 0:
                    for copy in arrivals(2):
                        copy.start()

    def spin_part(s):
        band = iota((1, comps * bands), 1) % bands
        masks = [
            jnp.where(band < occ_ref[s, k] - half * bands, 1.0, 0.0).astype(jnp.bfloat16)
            for k in range(kpts)
        ]

        def turned(t):
            for k in range(kpts):
                block_t = jnp.concatenate(
                    [x_ref[s, c, k, :, t * LANES : (t + 1) * LANES].T for c in range(comps)],
                    axis=1,
                )
                xt_ref[k, EDGE + t * LANES : EDGE + (t + 1) * LANES, :] = block_t * masks[k]

        arrived(s, 0)
        turned(0)
        for t in range(tiles):
            if t + 1 < tiles:
                arrived(s, t + 1)
                turned(t + 1)
            lane = iota((8, LANES), 1) + t * LANES
            rows = iota((8, LANES), 0)
            from_atom = rows - NPROJ * div18(lane)
            from_diagonal = rows - lane
            grams = []
            for k in range(kpts):
                real = x_ref[s, 0, k, :, t * LANES : (t + 1) * LANES]
                imag = x_ref[s, 1, k, :, t * LANES : (t + 1) * LANES]
                right = jnp.concatenate(
                    [
                        jnp.concatenate([real, imag], axis=1),
                        jnp.concatenate([imag, -real], axis=1),
                    ],
                    axis=0,
                )
                left = xt_ref[k, t * LANES : (t + 1) * LANES + 2 * EDGE, :]
                grams.append(dot_f32(left, right))
            first = t * LANES - EDGE
            sums = [None] * (FOLD // 8)
            for v in range((LANES + 2 * EDGE) // 8):
                row = first + 8 * v
                if row < 0 or row >= columns:
                    continue
                if row + 8 <= NPROJ * (t * LANES // NPROJ):
                    continue
                if row >= NPROJ * -(-(t + 1) * LANES // NPROJ):
                    continue
                if row < t * LANES:
                    parts = [g[8 * v : 8 * v + 8, :LANES] for g in grams]
                elif row >= (t + 1) * LANES:
                    parts = [g[8 * v : 8 * v + 8, LANES:] for g in grams]
                else:
                    upper = from_diagonal <= -row
                    parts = [
                        jnp.where(upper, g[8 * v : 8 * v + 8, :LANES], g[8 * v : 8 * v + 8, LANES:])
                        for g in grams
                    ]
                value = parts[0] * kw_ref[0]
                for k in range(1, kpts):
                    value = value + parts[k] * kw_ref[k]
                inside = (from_atom >= -row) & (from_atom < NPROJ - row)
                value = jnp.where(inside, value, 0.0)
                at = (row // 8) % (FOLD // 8)
                sums[at] = value if sums[at] is None else sums[at] + value
            for at, value in enumerate(sums):
                acc_ref[t, 8 * at : 8 * at + 8, :] = value
            folded = acc_ref[t, 0:24, :]
            for q in range(1, FOLD // NPROJ):
                folded = folded + acc_ref[t, NPROJ * q : NPROJ * q + 24, :]
            padded = jnp.concatenate([folded, jnp.zeros((LANES - 24, LANES), jnp.float32)], axis=0)
            y_ref[t * LANES : (t + 1) * LANES, :] = padded.T
        lane = iota((atoms, LANES), 1)
        packed = [jnp.zeros((atoms, LANES), jnp.float32) for _ in range(WIDE // LANES)]
        for j in range(NPROJ):
            piece = y_ref[pl.ds(j, atoms, stride=NPROJ), :]
            start = NPROJ * j
            shift = start % LANES
            if shift:
                piece = pltpu.roll(piece, shift, 1)
            tile = start // LANES
            here = (lane >= shift) & (lane < shift + NPROJ)
            packed[tile] = jnp.where(here, piece, packed[tile])
            if shift + NPROJ > LANES:
                packed[tile + 1] = jnp.where(lane < shift + NPROJ - LANES, piece, packed[tile + 1])
        high, low = split(jnp.concatenate(packed, axis=1))
        parts_ref[s] = jnp.concatenate([high, low], axis=0)

    for s in range(spins):
        spin_part(s)

    own = own_ref[...]
    row = jnp.sum(jnp.where(iota(own.shape, 0) == block // 2, own, 0), axis=0, keepdims=True)
    row = jnp.where(block % 2 == 1, pltpu.roll(row, LANES // 2, 1), row)
    eye = iota((atoms, LANES), 0) == iota((atoms, LANES), 1)
    rowf = row.astype(jnp.float32)
    col = jnp.sum(jnp.where(eye, rowf, 0.0), axis=1, keepdims=True)
    earlier = (col == rowf) & (iota((atoms, LANES), 0) < iota((atoms, LANES), 1))
    slot = jnp.sum(jnp.where(earlier, 1.0, 0.0), axis=0, keepdims=True)
    place = slot * 32.0 + rowf
    place = jnp.where(iota((1, LANES), 1) < atoms, place, pltpu.roll(place, atoms, 1))
    out_row = iota((LANES, LANES), 0).astype(jnp.float32)
    pick = jnp.concatenate(
        [
            jnp.where(place + 64.0 * s == out_row, 1.0, 0.0).astype(jnp.bfloat16)
            for s in range(spins)
        ],
        axis=1,
    )
    result = dot_f32(pick, parts_ref[...].reshape(spins * LANES, WIDE))
    owners = LANES // 4
    quarters = [result[owners * q : owners * (q + 1)] for q in range(4)]
    a0, a1, a2, a3 = [r[:, 2 * LANES :] for r in quarters]
    lane = iota((owners, LANES), 1)
    a1, a3 = pltpu.roll(a1, REST, 1), pltpu.roll(a3, 2 * REST - LANES + REST, 1)
    lines = [r[:, :LANES] for r in quarters] + [r[:, LANES : 2 * LANES] for r in quarters]
    lines += [
        jnp.where(lane < REST, a0, a1),
        jnp.where(
            lane < 2 * REST - LANES,
            a1,
            jnp.where(lane < 3 * REST - LANES, pltpu.roll(a2, 2 * REST - LANES, 1), a3),
        ),
        jnp.where(lane < 4 * REST - 2 * LANES, a3, 0.0),
    ]
    for n, line in enumerate(lines):
        out_ref[pl.ds(n, owners, stride=LINES), :] = line


def gram(index, occupied, kweights, owners, coefficients, interpret=False):
    spins, comps, kpts, bands, columns = coefficients.shape
    tiles = columns // LANES
    hbm = pl.BlockSpec(memory_space=pltpu.HBM)
    return pl.pallas_call(
        functools.partial(gram_kernel, index),
        in_specs=[hbm] * 4,
        out_specs=pl.BlockSpec(memory_space=pltpu.VMEM),
        out_shape=jax.ShapeDtypeStruct((LANES // 4 * LINES, LANES), jnp.float32),
        scratch_shapes=[
            pltpu.SMEM(occupied.shape, jnp.int32),
            pltpu.SMEM(kweights.shape, jnp.float32),
            pltpu.VMEM(owners.shape, jnp.int32),
            pltpu.VMEM(coefficients.shape, jnp.bfloat16),
            pltpu.VMEM((kpts, columns + 2 * EDGE, comps * bands), jnp.bfloat16),
            pltpu.VMEM((tiles, 80, LANES), jnp.float32),
            pltpu.VMEM((columns, LANES), jnp.float32),
            pltpu.VMEM((spins, LANES, WIDE), jnp.bfloat16),
            pltpu.SemaphoreType.DMA((3, comps, kpts)),
            pltpu.SemaphoreType.DMA((3,)),
        ],
        compiler_params=pltpu.CompilerParams(vmem_limit_bytes=GRAM_VMEM),
        cost_estimate=pl.CostEstimate(
            flops=2 * spins * kpts * columns * 160 * 2 * 2 * bands,
            bytes_accessed=spins * comps * kpts * bands * columns * 2,
            transcendentals=0,
        ),
        name="gram",
        interpret=interpret,
    )(occupied, kweights, owners, coefficients)


def sin_turns(t):
    t = t - jnp.floor(t + 0.5)
    t = jnp.where(t > 0.25, 0.5 - t, jnp.where(t < -0.25, -0.5 - t, t))
    x = t * np.float32(2.0 * np.pi)
    x2 = x * x
    p = np.float32(-1.0 / 39916800.0)
    for c in (1.0 / 362880.0, -1.0 / 5040.0, 1.0 / 120.0, -1.0 / 6.0):
        p = p * x2 + np.float32(c)
    return x + x * x2 * p


def signed(index):
    return jnp.where(index >= GRID // 2, index - GRID, index).astype(jnp.float32)


def wave_kernel(index, widths_ref, own_ref, species_ref, pos_ref, pot_ref, out_ref, kinds_ref, uh_ref, ul_ref):
    lines = 4
    rows = pot_ref.shape[0] // 6
    planes = rows * lines // GRID
    group = GRID // lines
    block, _, mine = index()
    own = own_ref[...]
    atoms = 16

    def spread(a):
        return jnp.concatenate([jnp.broadcast_to(a[r : r + 1], (4, LANES)) for r in range(4)], axis=0)

    at, lane16 = iota((atoms, LANES), 0), iota((atoms, LANES), 1)
    hit = (spread(own) == mine) & (lane16 // 64 == (at // 2) % 2)
    lanef = lane16.astype(jnp.float32)
    low = jnp.min(jnp.where(hit, lanef, 1e9), axis=1, keepdims=True)
    high = jnp.max(jnp.where(hit, lanef, -1.0), axis=1, keepdims=True)
    chosen = lanef == jnp.where(at % 2 == 1, high, low)

    lane = iota((1, LANES), 1)
    alpha, imag = (lane // atoms) % 4, lane // 64

    def on_lanes(a):
        column = jnp.sum(jnp.where(chosen, a, 0.0), axis=1, keepdims=True)
        return jnp.sum(jnp.where(at == lane16 % atoms, column, 0.0), axis=0, keepdims=True)

    place = [
        on_lanes(
            jnp.concatenate(
                [
                    jnp.broadcast_to(pos_ref[c : c + 1, r * LANES : (r + 1) * LANES], (4, LANES))
                    for r in range(4)
                ],
                axis=0,
            )
        )
        for c in range(3)
    ]
    kind = on_lanes(spread(species_ref[...]).astype(jnp.float32))
    width = jnp.where(kind > 0.5, widths_ref[0:1, 1:2], widths_ref[0:1, 0:1])
    turns = [p * np.float32(grid_step / (2.0 * np.pi)) for p in place]

    def power(g, exponent):
        g2 = g * g
        return jnp.where(
            exponent == 0, 1.0, jnp.where(exponent == 1, g, jnp.where(exponent == 2, g2, g2 * g))
        )

    mx = signed(iota((GRID, LANES), 0))
    gx = mx * grid_step
    phase = mx * turns[0]
    phase = phase - jnp.floor(phase + 0.5)
    factor = jnp.exp(-width * (gx * gx)) * power(gx, alpha)
    uh_ref[...] = jnp.zeros_like(uh_ref)
    ul_ref[...] = jnp.zeros_like(ul_ref)
    for c in range(2):
        shift = jnp.where(imag == 0, 0.25 + 0.25 * c, 0.25 * c)
        h, l = split(sin_turns(phase + shift) * factor)
        for line in range(lines):
            side, place_in = line // 2, line % 2
            r = c * 2 * LANES + line * GRID - side * LANES
            n = place_in * LANES
            uh_ref[side, r : r + GRID, n : n + LANES] = h
            ul_ref[side, r : r + GRID, n : n + LANES] = l

    def lines_of(low, high):
        pieces = [
            [
                split(pot_ref[pl.ds(2 * k + c + 6 * low, high - low, stride=6), :])
                for k in range(3)
            ]
            for c in range(2)
        ]
        sides = []
        for side in range(2):
            vh = jnp.concatenate([pieces[c][side + k][0] for c in range(2) for k in range(2)], axis=1)
            vl = jnp.concatenate([pieces[c][side + k][1] for c in range(2) for k in range(2)], axis=1)
            uh, ul = uh_ref[side], ul_ref[side]
            sides.append(dot_f32(vh, uh) + dot_f32(vl, uh) + dot_f32(vh, ul))
        return jnp.concatenate(sides, axis=1)

    def tiled(a):
        return jnp.concatenate([a] * lines, axis=1)

    my = signed(lines * iota((group, lines * LANES), 0) + iota((group, lines * LANES), 1) // LANES)
    gy = my * grid_step
    phase = my * tiled(turns[1])
    phase = phase - jnp.floor(phase + 0.5)
    shift = tiled(jnp.where(imag == 0, 0.0, 0.25))
    damp = jnp.exp(-tiled(width) * (gy * gy))
    y1 = sin_turns(phase + shift) * damp
    y2 = sin_turns(phase + shift + 0.25) * damp

    zi = iota((16, LANES), 0) + block * planes
    mz = signed(jnp.where(zi >= GRID, zi - GRID, zi))
    gz = mz * grid_step
    phase = mz * turns[2]
    phase = phase - jnp.floor(phase + 0.5)
    damp = jnp.exp(-width * (gz * gz))
    zs = sin_turns(phase) * damp
    zc = sin_turns(phase + 0.25) * damp

    sums = {}
    chunk = planes // CHUNKS
    for z in range(planes):
        if z % chunk == 0:
            first = lines_of(z * group, (z + chunk) * group)
        wave = y1 * tiled(zc[z : z + 1]) + y2 * tiled(zs[z : z + 1])
        row = z % chunk * group
        term = first[row : row + group] * wave
        gz_row = gz[z : z + 1]
        for b in range(4):
            if b:
                term = term * gy
            total = None
            for r in range(0, group, 8):
                for line in range(lines):
                    piece = term[r : r + 8, line * LANES : (line + 1) * LANES]
                    total = piece if total is None else total + piece
            for c in range(4 - b):
                if c:
                    total = total * gz_row
                sums[b, c] = total if z == 0 else sums[b, c] + total
    reduced = {k: jnp.sum(v, axis=0, keepdims=True) for k, v in sums.items()}
    which = iota((MONO_PAD, LANES), 0)
    table = jnp.zeros((MONO_PAD, LANES), jnp.float32)
    for m, (a, b, c) in enumerate(MONOMIALS):
        table = jnp.where((which == m) & (alpha == a), reduced[b, c], table)
    aux = jnp.where(which == 0, kind, 0.0)
    turned = jnp.concatenate([table, aux, jnp.zeros((64, LANES), jnp.float32)], axis=0).T
    result = turned[0:atoms]
    for g in range(1, LANES // atoms):
        result = result + turned[g * atoms : (g + 1) * atoms]
    lane = iota((atoms, LANES), 1)
    sent = jnp.where(lane < MONO_PAD, result, 0.0)
    kinds_ref[...] = result
    for row in range(4):
        line = sent[4 * row : 4 * row + 1]
        for k in range(1, 4):
            line = line + pltpu.roll(sent[4 * row + k : 4 * row + k + 1], MONO_PAD * k, 1)
        out_ref[row : row + 1, :] = line


def waves(index, widths, owners, species, positions, potential, interpret=False):
    vmem = pl.BlockSpec(memory_space=pltpu.VMEM)
    return pl.pallas_call(
        functools.partial(wave_kernel, index),
        in_specs=[vmem] * 5,
        out_specs=(vmem, vmem),
        out_shape=(
            jax.ShapeDtypeStruct((4, LANES), jnp.float32),
            jax.ShapeDtypeStruct((16, LANES), jnp.float32),
        ),
        scratch_shapes=[pltpu.VMEM((2, 4 * LANES, 2 * LANES), jnp.bfloat16)] * 2,
        cost_estimate=pl.CostEstimate(
            flops=2 * 288 * 768 * 512 * 3, bytes_accessed=potential.size * 4, transcendentals=0
        ),
        compiler_params=pltpu.CompilerParams(vmem_limit_bytes=16 << 20),
        name="waves",
        interpret=interpret,
    )(widths.reshape(1, -1), owners, species, positions, potential)


def final_kernel(index, parts_ref, sums_ref, kinds_ref, swap_ref, mult_ref, coef_ref, density_ref, forces_ref):
    senders = parts_ref.shape[0] // LINES
    sums_of = [
        jnp.sum(parts_ref[pl.ds(n, senders, stride=LINES), :], axis=0, keepdims=True)
        for n in range(LINES)
    ]
    lane = iota((1, LANES), 1)
    l8, l9, l10 = sums_of[8:]
    cut = 2 * LANES - 3 * REST
    ends = [
        l8,
        jnp.where(
            lane < LANES - REST, pltpu.roll(l8, LANES - REST, 1), pltpu.roll(l9, LANES - REST, 1)
        ),
        pltpu.roll(l9, 2 * LANES - 2 * REST, 1),
        jnp.where(lane < cut, pltpu.roll(l9, cut, 1), pltpu.roll(l10, cut, 1)),
    ]
    ends = [jnp.where(lane < REST, end, 0.0) for end in ends]
    at = iota((8, LANES), 0) % 4

    def stacked(rows):
        out = rows[3]
        for q in range(3):
            out = jnp.where(at == q, rows[q], out)
        return out

    z = jnp.concatenate([stacked(sums_of[0:4]), stacked(sums_of[4:8]), stacked(ends)], axis=1)
    swap = swap_ref[...]
    high = z.astype(jnp.bfloat16)
    rest = z - high.astype(jnp.float32)
    middle = rest.astype(jnp.bfloat16)
    low = (rest - middle.astype(jnp.float32)).astype(jnp.bfloat16)
    turned = dot_f32(high, swap) + dot_f32(middle, swap) + dot_f32(low, swap)
    e = iota((8, WIDE), 1)
    u = div18(e)
    v = e - NPROJ * u
    real = jnp.where(v <= u, z, turned)
    imag = jnp.where(u > v, turned, jnp.where(u < v, -z, 0.0))
    for s in range(2):
        density_ref[s, 0] = real[2 * s : 2 * s + 2, :PACKED]
        density_ref[s, 1] = imag[2 * s : 2 * s + 2, :PACKED]

    both = real + pltpu.roll(real, 2, 0)
    block = index()[0]
    line = jnp.broadcast_to(sums_ref[pl.ds(block // 2, 1), :], (8, LANES))
    lane, row = iota((8, LANES), 1), iota((8, LANES), 0)
    line = jnp.where(block % 2 == 1, pltpu.roll(line, 2 * MONO_PAD, 1), line)
    line = jnp.where(row % 2 == 1, pltpu.roll(line, 3 * MONO_PAD, 1), line)
    line = jnp.where(lane < MONO_PAD, line, 0.0)
    sums = line + pltpu.roll(line, MONO_PAD, 1) + pltpu.roll(line, 2 * MONO_PAD, 1)
    kinds = jnp.concatenate([kinds_ref[pl.ds(2 * block, 2), :]] * 4, axis=0)
    kind = jnp.sum(jnp.where(lane == MONO_PAD, kinds, 0.0), axis=1, keepdims=True) > 4.0
    poly = jnp.zeros((8, LANES), jnp.float32)
    for l in range(NL):
        chosen = jnp.where(kind, mult_ref[l, 1:2, :], mult_ref[l, 0:1, :])
        moment = jnp.sum(both[:, :PACKED] * chosen, axis=1, keepdims=True)
        poly = poly + moment * coef_ref[l : l + 1, :]
    terms = poly * sums
    forces = jnp.concatenate(
        [
            jnp.sum(jnp.where(lane // MONO_PAD == c, terms, 0.0), axis=1, keepdims=True)
            for c in range(3)
        ],
        axis=1,
    )
    forces_ref[...] = forces[0:2, :]


def final(index, parts, sums, kinds, swap, multipole, coefs, interpret=False):
    vmem = pl.BlockSpec(memory_space=pltpu.VMEM)
    return pl.pallas_call(
        functools.partial(final_kernel, index),
        in_specs=[vmem] * 6,
        out_specs=(vmem, vmem),
        out_shape=(
            jax.ShapeDtypeStruct((2, 2, 2, PACKED), jnp.float32),
            jax.ShapeDtypeStruct((2, 3), jnp.float32),
        ),
        cost_estimate=pl.CostEstimate(flops=10**7, bytes_accessed=10**5, transcendentals=0),
        compiler_params=pltpu.CompilerParams(vmem_limit_bytes=8 << 20),
        name="final",
        interpret=interpret,
    )(parts, sums, kinds, swap, multipole, coefs)


def place():
    half = lax.axis_index("ba")
    return lax.axis_index("ga"), half, lax.axis_index("ka") * lax.axis_size("ba") + half


def step(
    coefficients, occupied, kweights, owner_map, species, positions, multipole, widths, potential
):
    owners = owner_map.reshape(4, LANES)
    packed = gram(place, occupied, kweights, owners, coefficients)
    packed, widths, positions, species, potential, multipole = lax.optimization_barrier(
        (packed, widths, positions, species, potential, multipole)
    )
    packed = packed.reshape(-1, LINES, 1, LANES)
    arrived = lax.all_to_all(packed, ("ka", "ba"), split_axis=0, concat_axis=0, tiled=True)
    arrived = arrived.reshape(-1, LANES)
    values = potential.reshape(2, -1, LANES).transpose(1, 0, 2).reshape(-1, LANES)
    sums, kinds = waves(place, widths, owners, species.reshape(4, LANES), positions, values)
    sums = lax.psum(sums, "ga")
    density, forces = final(
        place,
        arrived,
        sums,
        kinds,
        jnp.asarray(swap_table(), jnp.bfloat16),
        multipole.transpose(1, 0, 2),
        jnp.asarray(force_coefficients()),
    )
    return density, forces.T


def solution(mesh):
    placed = (
        P(None, None, ("grp", "ka"), "ba", "ga"),
        P(None, ("grp", "ka")),
        P(("grp", "ka")),
        P("grp"),
        P("grp"),
        P(None, "grp"),
        P(),
        P(),
        P(None, ("grp", "ga")),
    )
    return jax.shard_map(
        step,
        mesh=mesh,
        in_specs=placed,
        out_specs=(
            P(None, None, ("grp", "ka", "ga", "ba"), None),
            P(None, ("grp", "ka", "ga", "ba")),
        ),
        check_vma=False,
    )
```
